256 devices in a mesh: aa: 64 (over y, z, core), ba: 4 (over x).
Axes of the slice: x: 4, y: 4, z: 8, core: 2. Of those that a mesh axis runs over, the one named last changes fastest.
Arguments:
- inputs: bfloat16 [32768, 3584], P('aa', 'ba'), may hold values from -6 to 6
- cotangent: bfloat16 [32768, 3584], P('aa', 'ba'), may hold values from -6 to 6
- base_weight: bfloat16 [3584, 3584], P(None, 'ba'), may hold values from -0.09375 to 0.09375
- adapter_ids: int32 [32768, 1], P('aa'), may hold values from 0 to 255; in each aligned block of 512 rows (0 to 511, 512 to 1023, ...) at most 4 rows name the same one
- adapters: float32 [256, 2, 16, 3584], P('aa', None, None, 'ba'), may hold values from -0.09375 to 0.09375
- first_moment: float32 [256, 2, 16, 3584], P('aa', None, None, 'ba'), may hold values from -3 to 3
- second_moment: float32 [256, 2, 16, 3584], P('aa', None, None, 'ba'), may hold values from 0.05 to 1
Outputs:
- input_gradient: bfloat16 [32768, 3584], P('aa', 'ba')
- new_adapters: float32 [256, 2, 16, 3584], P('aa', None, None, 'ba')
- new_first: float32 [256, 2, 16, 3584], P('aa', None, None, 'ba')
- new_second: float32 [256, 2, 16, 3584], P('aa', None, None, 'ba')
- grad_norm: float32 [], replicated
The draws below stay inside these ranges and needn't reach their ends.
Inputs may be any that keep to these rules, and one draw needn't show every extreme that they name: `adapter_ids`: in the rows of one device no adapter is named by more than 4 tokens, a bound that some block reaches; every adapter is named somewhere.
All inputs are finite; a program needn't handle non-finite values.
Results may differ from the reference program's by a relative error of at most 0.0034.
Values may be sent and summed in bfloat16 or wider, within the bound.
A program may use at most 128 MiB of HBM per device.

```python
import math
import jax
import jax.numpy as jnp
import numpy as np
from jax import lax

MODEL_WIDTH = 3584
R = 16
TOK_DEV = 512
ADAPTERS = 256
MOST = 4
TOKENS = 32768
N_AA = 64


def block_scale(stream_key, dims, cuts, smallest, largest):
    factor_of = 1.0
    for dim, blocks in cuts:
        steps = jax.random.uniform(jax.random.fold_in(jax.random.fold_in(stream_key, 6), dim), (blocks,), jnp.float32, smallest / len(cuts), largest / len(cuts))
        factor_of = factor_of * jnp.repeat(jnp.exp(steps), dims[dim] // blocks).reshape((-1,) + (1,) * (len(dims) - 1 - dim))
    return factor_of


def routed_block(stream_key, own, number, rows, count, top, limit, slope):
    sequence = jax.random.permutation(stream_key, count)
    crowded, ordinary = portions_of(count, rows * top, limit, slope, True), portions_of(count, rows * top, limit, slope, False)
    places = jnp.arange(count)

    def named(sizes, rotation):
        used = int((sizes > 0).sum())
        fixed = max(1, used // 4)
        moved = fixed + (places - fixed + rotation * (used - fixed)) % max(1, count - fixed)
        return jnp.zeros((count,), jnp.int32).at[sequence[jnp.where(places < fixed, places, moved)]].set(jnp.asarray(sizes, jnp.int32))

    sizes = jnp.where(number % 4 == 0, named(crowded, number // 4), named(ordinary, number - number // 4 - 1))
    mixed = jax.random.permutation(jax.random.fold_in(own, 3), count)
    giver, taker = mixed[0:count // 2 * 2:2], mixed[1:count // 2 * 2:2]
    room = jnp.minimum(sizes[giver] - 1, limit - sizes[taker]) // 2
    room = jnp.where((giver == sequence[0]) | (taker == sequence[0]) | (sizes[taker] == 0), 0, jnp.maximum(room, 0))
    moved = jax.random.randint(jax.random.fold_in(own, 4), (count // 2,), 0, 1 << 20) % (room + 1)
    sizes = sizes.at[giver].add(-moved).at[taker].add(moved)
    members = jnp.searchsorted(jnp.cumsum(sizes), jnp.arange(rows * top), side="right").astype(jnp.int32)
    table = members.reshape(top, rows).T
    table = table[jax.random.permutation(jax.random.fold_in(own, 1), rows)]
    rotation = jax.random.randint(jax.random.fold_in(own, 2), (rows, 1), 0, top)
    return jnp.take_along_axis(table, (jnp.arange(top)[None, :] + rotation) % top, axis=1)


def portions_of(number_of, total, reach, lean, full):
    portions = [(1 << 20) // math.isqrt(standing ** lean) + 1 for standing in range(1, number_of + 1)]
    largest = reach if full else min(reach, max(-(-total // number_of), total * portions[0] // sum(portions)))
    least = 1 if total - largest >= number_of - 1 else 0
    given, spare = [largest] + [least] * (number_of - 1), total - largest - least * (number_of - 1)
    while spare > 0:
        candidates = [i for i in range(1, number_of) if given[i] < largest] or [i for i in range(1, number_of) if given[i] < reach]
        pool, left = sum([portions[i] for i in candidates]), spare
        for i in candidates:
            addition = min(reach - given[i], max(1, left * portions[i] // pool), spare)
            given[i] = given[i] + addition
            spare = spare - addition
    return np.array(given)


def bell_draw(stream_key, extent, spread, reach, split=(), held_as=jnp.bfloat16):
    values = spread * jax.random.normal(stream_key, extent, jnp.float32)
    if split:
        values = values * block_scale(stream_key, extent, split, -0.22, 0.18)
    return jnp.clip(values, -reach, reach).astype(held_as)


def setup_inputs(seed: int = 0) -> dict:
    seeds = jax.random.split(jax.random.key(seed), 8)
    inputs = bell_draw(seeds[0], (TOKENS, MODEL_WIDTH), 1.0, 6.0, ((0, 64), (1, 4)))
    cotangent = bell_draw(seeds[1], (TOKENS, MODEL_WIDTH), 1.0, 6.0, ((0, 64), (1, 4)))
    base_weight = bell_draw(seeds[2], (MODEL_WIDTH, MODEL_WIDTH), MODEL_WIDTH ** -0.5, 0.09375, ((1, 4),))
    adapter_ids_keys = jax.random.split(jax.random.fold_in(seeds[3], 1), TOKENS // TOK_DEV)
    adapter_ids_turns = jax.random.permutation(jax.random.fold_in(seeds[3], 3), TOKENS // TOK_DEV)
    adapter_ids = jax.vmap(lambda own, number: routed_block(jax.random.fold_in(seeds[3], 2), own, number, TOK_DEV, ADAPTERS, 1, MOST, 2))(adapter_ids_keys, adapter_ids_turns).reshape((TOKENS, 1))
    adapters = bell_draw(seeds[4], (ADAPTERS, 2, R, MODEL_WIDTH), MODEL_WIDTH ** -0.5, 0.09375, ((0, 64), (3, 4)), jnp.float32)
    first_moment = bell_draw(seeds[5], (ADAPTERS, 2, R, MODEL_WIDTH), 0.2, 3.0, ((0, 64), (3, 4)), jnp.float32)
    second_moment = jnp.clip(jnp.exp(math.log(1.0) - 2.9957323 * jax.random.uniform(seeds[6], (ADAPTERS, 2, R, MODEL_WIDTH), jnp.float32) ** block_scale(seeds[6], (ADAPTERS, 2, R, MODEL_WIDTH), ((0, 64), (3, 4)), -0.2, 0.2)), 0.05, 1.0)
    return dict(inputs=inputs, cotangent=cotangent, base_weight=base_weight, adapter_ids=adapter_ids, adapters=adapters, first_moment=first_moment, second_moment=second_moment)


adapter_scale = 2.0
beta_first = 0.9
beta_second = 0.999
adam_eps = 1e-08
learn_rate = 0.01
bias_first = 1.0 - math.exp(1000.0 * math.log(beta_first))
bias_second = 1.0 - math.exp(1000.0 * math.log(beta_second))

def adam_update(adapters, first_moment, second_moment, gradients, squares):
    clip_limit = math.sqrt(2.0 * R * MODEL_WIDTH)
    clip_factor = clip_limit / jnp.maximum(jnp.sqrt(squares), clip_limit)
    clipped = gradients * clip_factor[:, None, None, None]
    new_first = beta_first * first_moment + (1.0 - beta_first) * clipped
    new_second = beta_second * second_moment + (1.0 - beta_second) * clipped * clipped
    update = new_first / bias_first / (jnp.sqrt(new_second / bias_second) + adam_eps)
    return (adapters - learn_rate * update, new_first, new_second)

def adapter_grouped(pieces):
    incoming_rows, cotangent_rows, down_full, up_full = pieces
    down_reduced = down_full.astype(jnp.bfloat16)
    up_low = up_full.astype(jnp.bfloat16)
    projected = jnp.dot(incoming_rows, down_reduced.T, preferred_element_type=jnp.float32)
    pulled = jnp.dot(cotangent_rows, up_low.T, preferred_element_type=jnp.float32)
    projection_reduced = projected.astype(jnp.bfloat16)
    fetched_reduced = pulled.astype(jnp.bfloat16)
    down_gradient = adapter_scale * jnp.dot(fetched_reduced.T, incoming_rows, preferred_element_type=jnp.float32)
    up_gradient = adapter_scale * jnp.dot(projection_reduced.T, cotangent_rows, preferred_element_type=jnp.float32)
    adapter_rows = (adapter_scale * jnp.dot(fetched_reduced, down_reduced, preferred_element_type=jnp.float32)).astype(jnp.bfloat16)
    return (down_gradient, up_gradient, adapter_rows)

def reference(inputs, cotangent, base_weight, adapter_ids, adapters, first_moment, second_moment):
    chosen = adapter_ids[:, 0].astype(jnp.int32)
    blocks = chosen.reshape(N_AA, TOK_DEV)
    counter = jnp.arange(TOK_DEV, dtype=jnp.int32)
    matches = (blocks[:, :, None] == blocks[:, None, :]) & (counter[None, None, :] < counter[None, :, None])
    slot_rank = lax.optimization_barrier(jnp.sum(matches.astype(jnp.int32), axis=2))
    block_index = jnp.arange(N_AA, dtype=jnp.int32)[:, None]
    token_position = (blocks * (N_AA * MOST) + block_index * MOST + slot_rank).reshape(-1).astype(jnp.int32)
    slot_overall = ADAPTERS * N_AA * MOST
    incoming_rows = jnp.zeros((slot_overall, MODEL_WIDTH), jnp.bfloat16).at[token_position].set(inputs).reshape(ADAPTERS, N_AA * MOST, MODEL_WIDTH)
    cotangent_rows = jnp.zeros((slot_overall, MODEL_WIDTH), jnp.bfloat16).at[token_position].set(cotangent).reshape(ADAPTERS, N_AA * MOST, MODEL_WIDTH)
    down_gradient, up_gradient, adapter_rows = lax.map(adapter_grouped, (incoming_rows, cotangent_rows, adapters[:, 0], adapters[:, 1]))
    adapter_local = adapter_rows.reshape(slot_overall, MODEL_WIDTH)[token_position]
    frozen_term = jnp.dot(cotangent, base_weight.T, preferred_element_type=jnp.float32)
    input_gradient = (frozen_term + adapter_local.astype(jnp.float32)).astype(jnp.bfloat16)
    gradients = jnp.stack([down_gradient, up_gradient], axis=1)
    squares = lax.optimization_barrier(jnp.sum(gradients * gradients, axis=(1, 2, 3)))
    new_adapters, new_first, new_second = adam_update(adapters, first_moment, second_moment, gradients, squares)
    return (input_gradient, new_adapters, new_first, new_second, jnp.sqrt(jnp.sum(squares)))
```

```python
import math

import jax
import jax.numpy as jnp
from jax import lax
from jax.experimental import pallas as pl
from jax.experimental.pallas import tpu as pltpu
from jax.sharding import PartitionSpec as P

MODEL_WIDTH = 3584
R = 16
NY, NZ, NC, NX = 4, 8, 2, 4
NK = 4
MOST = 4
GROUP = NY * NC
CHUNK = NZ * MOST
MESH = pl.DeviceIdType.MESH

adapter_scale = 2.0
beta_first = 0.9
beta_second = 0.999
adam_eps = 1e-08
learn_rate = 0.01
bias_first = 1.0 - math.exp(1000.0 * math.log(beta_first))
bias_second = 1.0 - math.exp(1000.0 * math.log(beta_second))

EX = ((2, 0), (2, 1), (1, 0), (3, 0), (1, 1), (3, 1), (0, 1))
ZOFF = (4, 3, 5, 2, 6, 1, 7)
XOFF = (2, 1, 3)


def adam_update(adapters, first_moment, second_moment, gradients, squares):
    clip_limit = math.sqrt(2.0 * R * MODEL_WIDTH)
    clip_factor = clip_limit / jnp.maximum(jnp.sqrt(squares), clip_limit)
    clipped = gradients * clip_factor[:, None, None, None]
    new_first = beta_first * first_moment + (1.0 - beta_first) * clipped
    new_second = beta_second * second_moment + (1.0 - beta_second) * clipped * clipped
    update = new_first / bias_first / (jnp.sqrt(new_second / bias_second) + adam_eps)
    return (adapters - learn_rate * update, new_first, new_second)


def nt(a, b):
    return lax.dot_general(a, b, (((1,), (1,)), ((), ())), preferred_element_type=jnp.float32)


def nn(a, b):
    return jnp.dot(a, b, preferred_element_type=jnp.float32)


def kernel(
    posr, posc, x_hbm, g_hbm, w_hbm, adf,
    out_ref, grad_ref, st_ref,
    xg, w, snd, rcv, adb, bs, br, acc, cs, cr, ls, lr, gs, gr, gf, sqs, sqr, ts, ty, us, tz,
    lsem, ex_s, ex_r, ag_s, ag_r, b_s, b_r, c_s, c_r, l_s, l_r, g_s, g_r, q_s, q_r, y_s, y_r, z_s, z_r,
):
    a = lax.axis_index("aa")
    x = lax.axis_index("ba")
    y, z, c = a // (NZ * NC), (a // NC) % NZ, a % NC
    me = y * NC + c
    fw = x_hbm.shape[1]

    def at_yc(dy, dc):
        yy, cc = (y + dy) % NY, (c + dc) % NC
        return yy * NC + cc, ((yy * NZ + z) * NC + cc, x)

    def at_z(dz):
        zz = (z + dz) % NZ
        return zz, ((y * NZ + zz) * NC + c, x)

    def at_x(dx):
        xx = (x + dx) % NX
        return xx, (a, xx)

    def remote(src, dst, ssem, rsem, dev):
        return pltpu.make_async_remote_copy(
            src_ref=src, dst_ref=dst, send_sem=ssem, recv_sem=rsem, device_id=dev, device_id_type=MESH
        )

    loads = [
        pltpu.make_async_copy(x_hbm, xg.at[:, 0:fw], lsem.at[0]),
        pltpu.make_async_copy(g_hbm, xg.at[:, fw : 2 * fw], lsem.at[1]),
        pltpu.make_async_copy(w_hbm, w, lsem.at[2]),
    ]
    for cp in loads:
        cp.start()

    barrier = pltpu.get_barrier_semaphore()
    for dy, dc in EX:
        pl.semaphore_signal(barrier, inc=1, device_id=at_yc(dy, dc)[1], device_id_type=MESH)
    for dz in ZOFF:
        pl.semaphore_signal(barrier, inc=1, device_id=at_z(dz)[1], device_id_type=MESH)
    for dx in XOFF:
        pl.semaphore_signal(barrier, inc=1, device_id=at_x(dx)[1], device_id_type=MESH)

    for k in range(NK):
        adb[k, z] = adf[k].astype(jnp.bfloat16)

    def ex_copy(k, j):
        d, dev = at_yc(*EX[j])
        return remote(snd.at[k, d], rcv.at[k, me], ex_s.at[k, j], ex_r.at[k, j], dev)

    def lora_copy(k, j):
        d, dev = at_yc(*EX[j])
        return remote(ls.at[k, d], lr.at[k, me], l_s.at[k, j], l_r.at[k, j], dev)

    def ag_copy(k, s, up):
        if up:
            o = (z - s + NZ) % NZ
            return remote(adb.at[k, o], adb.at[k, o], ag_s.at[k, s], ag_r.at[k, s], at_z(1)[1])
        o = (z + s) % NZ
        return remote(adb.at[k, o], adb.at[k, o], ag_s.at[k, 4 + s], ag_r.at[k, 4 + s], at_z(NZ - 1)[1])

    def g_copy(k, j):
        zz, dev = at_z(ZOFF[j])
        return remote(gs.at[k, zz], gr.at[k, j], g_s.at[k, j], g_r.at[k, j], dev)

    def base_copy(k, j):
        return remote(bs.at[k, j], br.at[k, j], b_s.at[k, j], b_r.at[k, j], at_x(XOFF[j])[1])

    def c_copy(k, j):
        return remote(cs.at[k], cr.at[k, x], c_s.at[k, j], c_r.at[k, j], at_x(XOFF[j])[1])

    def gather(k):
        rows = lax.broadcasted_iota(jnp.int32, (GROUP * CHUNK, 1), 0) + k * (GROUP * CHUNK)
        hot = jnp.where(rows == posr[...], 1.0, 0.0).astype(jnp.bfloat16)
        got = nn(hot, xg[...]).astype(jnp.bfloat16).reshape(GROUP, CHUNK, 2 * fw)
        snd[k] = got
        rcv[k, me] = snd[k, me]

    def send_tokens(k):
        for j in range(len(EX)):
            ex_copy(k, j).start()

    def base(k):
        rows = acc.shape[0] // NK
        here = pl.ds(pl.multiple_of(k * rows, rows), rows)
        g = xg[here, fw : 2 * fw]
        for j, dx in enumerate(XOFF):
            xx = at_x(dx)[0]
            part = nt(g, w[pl.ds(pl.multiple_of(xx * fw, fw), fw), :])
            bs[k, j] = part.astype(jnp.bfloat16)
            base_copy(k, j).start()
        acc[here, :] = nt(g, w[pl.ds(pl.multiple_of(x * fw, fw), fw), :])

    loads[0].wait()
    loads[1].wait()
    gather(0)
    pl.semaphore_wait(barrier, len(EX) + len(ZOFF) + len(XOFF))

    def ag_ways(k, s):
        return [up for up in (True, False) if s < 3 or up == (k % 2 == 0)]

    def ag_pass(s):
        for k in range(NK):
            for up in ag_ways(k, s):
                if s > 0:
                    ag_copy(k, s - 1, up).wait_recv()
                ag_copy(k, s, up).start()

    ag_pass(0)
    send_tokens(0)

    def feed(k, carry):
        gather(k)
        send_tokens(k)
        return carry

    lax.fori_loop(1, NK, feed, 0)
    ag_pass(1)
    loads[2].wait()
    base(0)
    ag_pass(2)
    ag_pass(3)
    for k in range(NK):
        for up in (True, False):
            last = 3 if up in ag_ways(k, 3) else 2
            for s in ((last,) if last == 3 else ()):
                ag_copy(k, s, up).wait_recv()
            if last == 2:
                ag_copy(k, 2, up).wait_recv()

    lane = lax.broadcasted_iota(jnp.int32, (1, NZ, NZ * R), 2) // R
    sub = lax.broadcasted_iota(jnp.int32, (1, NZ, NZ * R), 1)
    mine = lane == sub
    nrow = GROUP * CHUNK

    def step(k, carry):
        for j in range(len(EX)):
            ex_copy(k, j).wait_recv()
        down = adb[k, :, 0].reshape(NZ * R, fw)
        up = adb[k, :, 1].reshape(NZ * R, fw)
        xs = rcv[k, :, :, 0:fw].reshape(nrow, fw)
        gg = rcv[k, :, :, fw : 2 * fw].reshape(nrow, fw)
        pulled = nt(gg, up).reshape(GROUP * MOST, NZ, NZ * R)
        projected = nt(xs, down).reshape(GROUP * MOST, NZ, NZ * R)
        cs[k, 0] = jnp.sum(jnp.where(mine, pulled, 0.0), axis=1)
        cs[k, 1] = jnp.sum(jnp.where(mine, projected, 0.0), axis=1)
        cr[k, x] = cs[k]
        for j in range(len(XOFF)):
            c_copy(k, j).start()

        @pl.when(k < NK - 1)
        def _():
            base(k + 1)

        for j in range(len(XOFF)):
            c_copy(k, j).wait_recv()
        total = cr[k, 0] + cr[k, 1] + cr[k, 2] + cr[k, 3]
        low = total.astype(jnp.bfloat16).astype(jnp.float32)
        pull = jnp.where(mine, low[0][:, None, :], 0.0).reshape(nrow, NZ * R)
        proj = jnp.where(mine, low[1][:, None, :], 0.0).reshape(nrow, NZ * R)
        gd = adapter_scale * nn(pull.T.astype(jnp.bfloat16), xs)
        gu = adapter_scale * nn(proj.T.astype(jnp.bfloat16), gg)
        gf[:, 0] = gd.reshape(NZ, R, fw)
        gf[:, 1] = gu.reshape(NZ, R, fw)
        gs[k, :, 0] = gd.reshape(NZ, R, fw).astype(jnp.bfloat16)
        gs[k, :, 1] = gu.reshape(NZ, R, fw).astype(jnp.bfloat16)
        for j in range(len(ZOFF)):
            g_copy(k, j).start()
        grad_ref[k] = gf[z]
        lora = adapter_scale * nn(pull.astype(jnp.bfloat16), down)
        ls[k] = lora.astype(jnp.bfloat16).reshape(GROUP, CHUNK, fw)
        for j in range(len(EX)):
            lora_copy(k, j).start()
        lr[k, me] = ls[k, me]
        return carry

    lax.fori_loop(0, NK, step, 0)

    def frozen(k, carry):
        rows = acc.shape[0] // NK
        here = pl.ds(pl.multiple_of(k * rows, rows), rows)
        t = acc[here, :]
        for j in range(len(XOFF)):
            base_copy(k, j).wait_recv()
        for j in range(len(XOFF)):
            t = t + br[k, j].astype(jnp.float32)
        acc[here, :] = t
        return carry

    lax.fori_loop(0, NK, frozen, 0)

    def unslot(k, carry):
        for j in range(len(EX)):
            lora_copy(k, j).wait_recv()
        cols = lax.broadcasted_iota(jnp.int32, (1, nrow), 1) + k * nrow
        hot = jnp.where(posc[...] == cols, 1.0, 0.0).astype(jnp.bfloat16)
        acc[...] += nn(hot, lr[k].reshape(nrow, fw))
        return carry

    lax.fori_loop(0, NK, unslot, 0)
    out_ref[...] = acc[...].astype(jnp.bfloat16)

    row = lax.broadcasted_iota(jnp.int32, (8, 128), 0)

    def total_gradient(k, sq):
        for j in range(len(ZOFF)):
            g_copy(k, j).wait_recv()
        t = grad_ref[k]
        for j in range(len(ZOFF)):
            t = t + gr[k, j].astype(jnp.float32)
        grad_ref[k] = t
        return sq + jnp.where(row == k, jnp.sum(t * t), 0.0)

    sqs[...] = lax.fori_loop(0, NK, total_gradient, jnp.zeros((8, 128), jnp.float32))

    def q_copy(j):
        return remote(sqs, sqr.at[x], q_s.at[j], q_r.at[j], at_x(XOFF[j])[1])

    sqr[x] = sqs[...]
    for j in range(len(XOFF)):
        q_copy(j).start()
    for j in range(len(XOFF)):
        q_copy(j).wait_recv()
    squares = sqr[0] + sqr[1] + sqr[2] + sqr[3]

    def y_copy(j):
        return remote(ts, ty.at[me], y_s.at[j], y_r.at[j], at_yc(*EX[j])[1])

    ts[...] = jnp.broadcast_to(jnp.sum(squares, axis=0, keepdims=True), (8, 128))
    ty[me] = ts[...]
    for j in range(len(EX)):
        y_copy(j).start()
    for j in range(len(EX)):
        y_copy(j).wait_recv()

    def z_copy(j):
        return remote(us, tz.at[z], z_s.at[j], z_r.at[j], at_z(ZOFF[j])[1])

    us[...] = jnp.sum(ty[...], axis=0)
    tz[z] = us[...]
    for j in range(len(ZOFF)):
        z_copy(j).start()
    for j in range(len(ZOFF)):
        z_copy(j).wait_recv()
    st_ref[...] = jnp.where(row == NK, jnp.sum(tz[...], axis=0), squares)

    def done(k, carry):
        for j in range(len(EX)):
            ex_copy(k, j).wait_send()
            lora_copy(k, j).wait_send()
        for j in range(len(ZOFF)):
            g_copy(k, j).wait_send()
        for j in range(len(XOFF)):
            base_copy(k, j).wait_send()
            c_copy(k, j).wait_send()
        return carry

    lax.fori_loop(0, NK, done, 0)
    for k in range(NK):
        for s in range(4):
            for up in ag_ways(k, s):
                ag_copy(k, s, up).wait_send()
    for j in range(len(XOFF)):
        q_copy(j).wait_send()
    for j in range(len(EX)):
        y_copy(j).wait_send()
    for j in range(len(ZOFF)):
        z_copy(j).wait_send()


def local(inputs, cotangent, base_weight, adapter_ids, adapters, first_moment, second_moment):
    tok, fw = inputs.shape
    chosen = adapter_ids[:, 0]
    counter = jnp.arange(tok, dtype=jnp.int32)
    matches = (chosen[:, None] == chosen[None, :]) & (counter[None, :] < counter[:, None])
    rank = jnp.sum(matches.astype(jnp.int32), axis=1)
    k = chosen % NK
    core = chosen // NK % NC
    zz = chosen // (NK * NC) % NZ
    yy = chosen // (NK * NC * NZ)
    pos = ((k * GROUP + yy * NC + core) * MOST + rank) * NZ + zz
    bf, f32 = jnp.bfloat16, jnp.float32
    dma = pltpu.SemaphoreType.DMA
    vm, hbm = pl.BlockSpec(memory_space=pltpu.VMEM), pl.BlockSpec(memory_space=pl.ANY)
    out, gradients, stats = pl.pallas_call(
        kernel,
        out_shape=(
            jax.ShapeDtypeStruct((tok, fw), bf),
            jax.ShapeDtypeStruct((NK, 2, R, fw), f32),
            jax.ShapeDtypeStruct((8, 128), f32),
        ),
        in_specs=[vm, vm, hbm, hbm, hbm, vm],
        out_specs=(vm, vm, vm),
        scratch_shapes=[
            pltpu.VMEM((tok, 2 * fw), bf),
            pltpu.VMEM(base_weight.shape, bf),
            pltpu.VMEM((NK, GROUP, CHUNK, 2 * fw), bf),
            pltpu.VMEM((NK, GROUP, CHUNK, 2 * fw), bf),
            pltpu.VMEM((NK, NZ, 2, R, fw), bf),
            pltpu.VMEM((NK, 3, tok // NK, fw), bf),
            pltpu.VMEM((NK, 3, tok // NK, fw), bf),
            pltpu.VMEM((tok, fw), f32),
            pltpu.VMEM((NK, 2, GROUP * MOST, NZ * R), f32),
            pltpu.VMEM((NK, NX, 2, GROUP * MOST, NZ * R), f32),
            pltpu.VMEM((NK, GROUP, CHUNK, fw), bf),
            pltpu.VMEM((NK, GROUP, CHUNK, fw), bf),
            pltpu.VMEM((NK, NZ, 2, R, fw), bf),
            pltpu.VMEM((NK, NZ - 1, 2, R, fw), bf),
            pltpu.VMEM((NZ, 2, R, fw), f32),
            pltpu.VMEM((8, 128), f32),
            pltpu.VMEM((NX, 8, 128), f32),
            pltpu.VMEM((8, 128), f32),
            pltpu.VMEM((GROUP, 8, 128), f32),
            pltpu.VMEM((8, 128), f32),
            pltpu.VMEM((NZ, 8, 128), f32),
            dma((3,)),
            dma((NK, 7)), dma((NK, 7)),
            dma((NK, 8)), dma((NK, 8)),
            dma((NK, 3)), dma((NK, 3)),
            dma((NK, 3)), dma((NK, 3)),
            dma((NK, 7)), dma((NK, 7)),
            dma((NK, 7)), dma((NK, 7)),
            dma((3,)), dma((3,)),
            dma((7,)), dma((7,)),
            dma((7,)), dma((7,)),
        ],
        compiler_params=pltpu.CompilerParams(
            collective_id=0, has_side_effects=True, vmem_limit_bytes=60 * 1024 * 1024
        ),
    )(pos[None, :], pos[:, None], inputs, cotangent, base_weight, adapters)
    new_adapters, new_first, new_second = adam_update(
        adapters, first_moment, second_moment, gradients, stats[:NK, 0]
    )
    return (out, new_adapters, new_first, new_second, jnp.sqrt(stats[NK, 0]))


def solution(mesh):
    in_specs = (
        P("aa", "ba"),
        P("aa", "ba"),
        P(None, "ba"),
        P("aa", None),
        P("aa", None, None, "ba"),
        P("aa", None, None, "ba"),
        P("aa", None, None, "ba"),
    )
    out_specs = (
        P("aa", "ba"),
        P("aa", None, None, "ba"),
        P("aa", None, None, "ba"),
        P("aa", None, None, "ba"),
        P(),
    )
    return jax.shard_map(local, mesh=mesh, in_specs=in_specs, out_specs=out_specs, check_vma=False)
```

```python
import math

import jax
import jax.numpy as jnp
from jax import lax
from jax.experimental import pallas as pl
from jax.experimental.pallas import tpu as pltpu
from jax.sharding import PartitionSpec as P

MODEL_WIDTH = 3584
R = 16
NY, NZ, NC, NX = 4, 8, 2, 4
NK = 4
MOST = 4
GROUP = NY * NC
CHUNK = NZ * MOST
MESH = pl.DeviceIdType.MESH

adapter_scale = 2.0
beta_first = 0.9
beta_second = 0.999
adam_eps = 1e-08
learn_rate = 0.01
bias_first = 1.0 - math.exp(1000.0 * math.log(beta_first))
bias_second = 1.0 - math.exp(1000.0 * math.log(beta_second))

EX = ((2, 0), (2, 1), (1, 0), (3, 0), (1, 1), (3, 1), (0, 1))
ZOFF = (4, 3, 5, 2, 6, 1, 7)
XOFF = (2, 1, 3)
f32, bf16, i32 = jnp.float32, jnp.bfloat16, jnp.int32


def nt(a, b):
    return lax.dot_general(a, b, (((1,), (1,)), ((), ())), preferred_element_type=f32)


def nn(a, b):
    return jnp.dot(a, b, preferred_element_type=f32)


def kernel(
    ids, x_hbm, g_hbm, w_hbm, ad_hbm,
    out_hbm, grad_hbm, st_ref,
    adf, posr, posc, xg, w, snd, rcv, adb, bs, br, acc, cs, cr, ls, lr, gs, gf, hs, hr, hq, gr, gown, obf,
    sqs, sqr, ts, ty, us, tz,
    lsem, osem, ex_s, ex_r, ag_s, ag_r, b_s, b_r, c_s, c_r, l_s, l_r, g_s, g_r, q_s, q_r, y_s, y_r, z_s, z_r,
):
    a = lax.axis_index("aa")
    x = lax.axis_index("ba")
    y, z, c = a // (NZ * NC), (a // NC) % NZ, a % NC
    me = y * NC + c
    tok, fw = x_hbm.shape
    nrow = GROUP * CHUNK
    quarter = tok // NK

    def at_yc(dy, dc):
        yy, cc = (y + dy) % NY, (c + dc) % NC
        return yy * NC + cc, ((yy * NZ + z) * NC + cc, x)

    def at_z(dz):
        zz = (z + dz + NZ) % NZ
        return zz, ((y * NZ + zz) * NC + c, x)

    def at_x(dx):
        xx = (x + dx) % NX
        return xx, (a, xx)

    barrier = pltpu.get_barrier_semaphore()
    for dz in ZOFF:
        pl.semaphore_signal(barrier, inc=1, device_id=at_z(dz)[1], device_id_type=MESH)
    for dy, dc in EX:
        pl.semaphore_signal(barrier, inc=1, device_id=at_yc(dy, dc)[1], device_id_type=MESH)
    for dx in XOFF:
        pl.semaphore_signal(barrier, inc=1, device_id=at_x(dx)[1], device_id_type=MESH)

    loads = [
        pltpu.make_async_copy(ad_hbm, adf, lsem.at[0]),
        pltpu.make_async_copy(x_hbm, xg.at[:, 0:fw], lsem.at[1]),
        pltpu.make_async_copy(g_hbm, xg.at[:, fw : 2 * fw], lsem.at[2]),
        pltpu.make_async_copy(w_hbm, w, lsem.at[3]),
    ]
    for cp in loads:
        cp.start()

    def remote(src, dst, ssem, rsem, dev):
        return pltpu.make_async_remote_copy(
            src_ref=src, dst_ref=dst, send_sem=ssem, recv_sem=rsem, device_id=dev, device_id_type=MESH
        )

    def ex_copy(k, j):
        d, dev = at_yc(*EX[j])
        return remote(snd.at[k, d], rcv.at[k, me], ex_s.at[k, j], ex_r.at[k, j], dev)

    def lora_copy(k, j):
        d, dev = at_yc(*EX[j])
        return remote(ls.at[k, d], lr.at[k, me], l_s.at[k, j], l_r.at[k, j], dev)

    def ag_copy(k, s, up):
        o, i = at_z(-s if up else s)[0], s if up else 4 + s
        return remote(adb.at[k, o], adb.at[k, o], ag_s.at[k, i], ag_r.at[k, i], at_z(1 if up else -1)[1])

    def g_copy(k, j):
        side = 1 if j % 2 == 0 else -1
        if j < 2:
            src, dst, to = gs.at[k, at_z(side)[0]], gr.at[k, j], side
        elif j < 4:
            src, dst, to = gs.at[k, at_z(3 * side)[0]], hr.at[k, j - 2], side
        elif j < 6:
            src, dst, to = gs.at[k, at_z(4)[0], j - 4], hq.at[k, j - 4], 2 * side
        else:
            src, dst, to = hs.at[k, j - 6], gr.at[k, j - 4], 2 * side
        return remote(src, dst, g_s.at[k, j], g_r.at[k, j], at_z(to)[1])

    def base_copy(q, j):
        here = pl.ds(q * quarter, quarter)
        return remote(bs.at[j, here, :], br.at[j, here, :], b_s.at[q, j], b_r.at[q, j], at_x(XOFF[j])[1])

    def c_copy(k, j):
        return remote(cs.at[k], cr.at[k, x], c_s.at[k, j], c_r.at[k, j], at_x(XOFF[j])[1])

    def q_copy(j):
        return remote(sqs, sqr.at[x], q_s.at[j], q_r.at[j], at_x(XOFF[j])[1])

    def y_copy(j):
        return remote(ts, ty.at[me], y_s.at[j], y_r.at[j], at_yc(*EX[j])[1])

    def z_copy(j):
        return remote(us, tz.at[z], z_s.at[j], z_r.at[j], at_z(ZOFF[j])[1])

    def positions():
        row = ids[...]
        col = jnp.broadcast_to(row, (128, tok)).T[:, 0:1]
        before = lax.broadcasted_iota(i32, (tok, 1), 0) < lax.broadcasted_iota(i32, (1, tok), 1)
        rank = jnp.sum(jnp.where((col == row) & before, 1, 0), axis=0, keepdims=True)
        k, core = row & (NK - 1), (row >> 2) & (NC - 1)
        zz, yy = (row >> 3) & (NZ - 1), row >> 6
        pos = ((k * GROUP + yy * NC + core) * MOST + rank) * NZ + zz
        posr[...] = pos
        posc[...] = jnp.broadcast_to(pos, (128, tok)).T

    def gather(k):
        rows = lax.broadcasted_iota(i32, (nrow, 1), 0) + k * nrow
        hot = jnp.where(rows == posr[...], 1.0, 0.0).astype(bf16)
        snd[k] = nn(hot, xg[...]).astype(bf16).reshape(GROUP, CHUNK, 2 * fw)
        rcv[k, me] = snd[k, me]

    def send_tokens(k):
        for j in range(len(EX)):
            ex_copy(k, j).start()

    def frozen_of(dx):
        xx = at_x(dx)[0]
        return nt(xg[:, fw : 2 * fw], w[pl.ds(pl.multiple_of(xx * fw, fw), fw), :])

    def frozen_for(j):
        bs[j] = frozen_of(XOFF[j]).astype(bf16)

    def ag_ways(k, s):
        return [up for up in (True, False) if s < 3 or up == (k % 2 == 0)]

    def ag_pass(k, s):
        for up in ag_ways(k, s):
            if s > 0:
                ag_copy(k, s - 1, up).wait_recv()
            ag_copy(k, s, up).start()

    def ag_end(k):
        for up in (True, False):
            ag_copy(k, 3 if up in ag_ways(k, 3) else 2, up).wait_recv()

    lane = lax.broadcasted_iota(i32, (1, NZ, NZ * R), 2) // R
    sub = lax.broadcasted_iota(i32, (1, NZ, NZ * R), 1)
    mine = lane == sub

    def rows_of(k, first):
        return rcv[k, :, :, first : first + fw].reshape(nrow, fw)

    def project(k):
        pulled = nt(rows_of(k, fw), adb[k, :, 1].reshape(NZ * R, fw)).reshape(GROUP * MOST, NZ, NZ * R)
        projected = nt(rows_of(k, 0), adb[k, :, 0].reshape(NZ * R, fw)).reshape(GROUP * MOST, NZ, NZ * R)
        cs[k, 0] = jnp.sum(jnp.where(mine, pulled, 0.0), axis=1)
        cs[k, 1] = jnp.sum(jnp.where(mine, projected, 0.0), axis=1)
        cr[k, x] = cs[k]
        for j in range(len(XOFF)):
            c_copy(k, j).start()

    def gradients(k):
        low = (cr[k, 0] + cr[k, 1] + cr[k, 2] + cr[k, 3]).astype(bf16).astype(f32)
        pull = jnp.where(mine, low[0][:, None, :], 0.0).reshape(nrow, NZ * R)
        proj = jnp.where(mine, low[1][:, None, :], 0.0).reshape(nrow, NZ * R)
        for i, (side, first) in enumerate(((pull, 0), (proj, fw))):
            grad = (adapter_scale * nn(side.T.astype(bf16), rows_of(k, first))).reshape(NZ, R, fw)
            gf[:, i] = grad
            gs[k, :, i] = grad.astype(bf16)
        for j in (2, 3, 4, 5, 0, 1):
            g_copy(k, j).start()
        gown[k] = gf[z]
        lora = adapter_scale * nn(pull.astype(bf16), adb[k, :, 0].reshape(NZ * R, fw))
        ls[k] = lora.astype(bf16).reshape(GROUP, CHUNK, fw)
        for j in range(len(EX)):
            lora_copy(k, j).start()
        lr[k, me] = ls[k, me]

    def hub(k):
        for side in range(2):
            g_copy(k, 2 + side).wait_recv()
            g_copy(k, 4 + side).wait_recv()
            sign = 1 if side == 0 else -1
            for i in range(2):
                t = gf[at_z(2 * sign)[0], i] + hr[k, side, i].astype(f32)
                if i == side:
                    t = t + hq[k, side].astype(f32)
                hs[k, side, i] = t.astype(bf16)
            g_copy(k, 6 + side).start()

    def unslot(k):
        cols = lax.broadcasted_iota(i32, (1, nrow), 1) + k * nrow
        hot = jnp.where(posc[:, 0:1] == cols, 1.0, 0.0).astype(bf16)
        acc[...] += nn(hot, lr[k].reshape(nrow, fw))

    def total_gradient(k):
        for j in (0, 1, 6, 7):
            g_copy(k, j).wait_recv()
        t = gown[k]
        for j in range(4):
            t = t + gr[k, j].astype(f32)
        gown[k] = t
        return jnp.sum(t * t)

    for k in range(NK):
        if k == 0:
            loads[0].wait()
        adb[k, z] = adf[k].astype(bf16)
    positions()
    loads[1].wait()
    loads[2].wait()
    for k in range(NK):
        gather(k)
    loads[3].wait()
    frozen_for(0)
    pl.semaphore_wait(barrier, len(EX) + len(ZOFF) + len(XOFF))

    ag_pass(0, 0)
    send_tokens(0)
    base_copy(0, 0).start()
    ag_pass(1, 0)
    for k in range(1, NK):
        send_tokens(k)
    frozen_for(1)
    base_copy(0, 1).start()
    ag_pass(0, 1)
    ag_pass(2, 0)
    frozen_for(2)
    base_copy(0, 2).start()
    base_copy(1, 0).start()
    ag_pass(1, 1)
    ag_pass(0, 2)
    ag_pass(3, 0)
    ag_pass(2, 1)
    ag_pass(1, 2)
    ag_pass(0, 3)
    acc[...] = frozen_of(0)
    ag_pass(3, 1)
    ag_pass(2, 2)
    ag_pass(1, 3)
    ag_end(0)

    later = ([(1, 1), (1, 2)], [(2, 0), (2, 1), (2, 2)], [(3, 0)], [(3, 1), (3, 2)])
    for k in range(NK):
        if k > 0:
            ag_end(k)
        for j in range(len(EX)):
            ex_copy(k, j).wait_recv()
        project(k)
        for q, j in later[k]:
            base_copy(q, j).start()
        if k == 0:
            ag_pass(3, 2)
            ag_pass(2, 3)
            ag_pass(3, 3)
        else:
            hub(k - 1)
        for j in range(len(XOFF)):
            c_copy(k, j).wait_recv()
        gradients(k)

    def frozen(q):
        here = pl.ds(q * quarter, quarter)
        for j in range(len(XOFF)):
            base_copy(q, j).wait_recv()
        t = acc[here, :]
        for j in range(len(XOFF)):
            t = t + br[j, here, :].astype(f32)
        acc[here, :] = t

    def lora_wait(k):
        for j in range(len(EX)):
            lora_copy(k, j).wait_recv()

    frozen(0)
    frozen(1)
    lora_wait(0)
    unslot(0)
    hub(NK - 1)
    frozen(2)
    lora_wait(1)
    unslot(1)
    row = lax.broadcasted_iota(i32, (8, 128), 0)
    sq = jnp.zeros((8, 128), f32)
    for k in range(NK):
        sq = sq + jnp.where(row == k, total_gradient(k), 0.0)
    sqs[...] = sq
    for j in range(len(XOFF)):
        q_copy(j).start()
    sqr[x] = sq
    grad_out = pltpu.make_async_copy(gown, grad_hbm, osem.at[0])
    grad_out.start()
    frozen(3)
    lora_wait(2)
    unslot(2)
    for j in range(len(XOFF)):
        q_copy(j).wait_recv()
    squares = sqr[0] + sqr[1] + sqr[2] + sqr[3]
    ts[...] = jnp.broadcast_to(jnp.sum(squares, axis=0, keepdims=True), (8, 128))
    for j in range(len(EX)):
        y_copy(j).start()
    ty[me] = ts[...]
    for j in range(len(EX)):
        y_copy(j).wait_recv()
    us[...] = jnp.sum(ty[...], axis=0)
    for j in range(len(ZOFF)):
        z_copy(j).start()
    tz[z] = us[...]
    lora_wait(3)
    unslot(3)
    obf[...] = acc[...].astype(bf16)
    out_copy = pltpu.make_async_copy(obf, out_hbm, osem.at[1])
    out_copy.start()
    for k in range(NK):
        for j in range(len(EX)):
            ex_copy(k, j).wait_send()
            lora_copy(k, j).wait_send()
        for j in range(8):
            g_copy(k, j).wait_send()
        for j in range(len(XOFF)):
            base_copy(k, j).wait_send()
            c_copy(k, j).wait_send()
        for s in range(4):
            for up in ag_ways(k, s):
                ag_copy(k, s, up).wait_send()
    for j in range(len(XOFF)):
        q_copy(j).wait_send()
    for j in range(len(EX)):
        y_copy(j).wait_send()
    for j in range(len(ZOFF)):
        z_copy(j).wait_recv()
    st_ref[...] = jnp.where(row == NK, jnp.sum(tz[...], axis=0), squares)
    for j in range(len(ZOFF)):
        z_copy(j).wait_send()
    grad_out.wait()
    out_copy.wait()


def finish(out_ref, grad_ref, st_ref, ad_ref, m_ref, v_ref, o_ref, na_ref, nf_ref, ns_ref, norm_ref):
    clip_limit = math.sqrt(2.0 * R * MODEL_WIDTH)
    o_ref[...] = out_ref[...]
    for k in range(NK):
        factor = clip_limit / jnp.maximum(jnp.sqrt(st_ref[k : k + 1, 0:1]), clip_limit)
        clipped = grad_ref[k] * factor
        new_first = beta_first * m_ref[k] + (1.0 - beta_first) * clipped
        new_second = beta_second * v_ref[k] + (1.0 - beta_second) * clipped * clipped
        update = new_first / bias_first / (jnp.sqrt(new_second / bias_second) + adam_eps)
        na_ref[k] = ad_ref[k] - learn_rate * update
        nf_ref[k] = new_first
        ns_ref[k] = new_second
    norm_ref[...] = jnp.sqrt(st_ref[NK : NK + 1, 0:1])


def local(inputs, cotangent, base_weight, adapter_ids, adapters, first_moment, second_moment):
    tok, fw = inputs.shape
    dma = pltpu.SemaphoreType.DMA
    vm, hbm = pl.BlockSpec(memory_space=pltpu.VMEM), pl.BlockSpec(memory_space=pl.ANY)
    own = (NK, 2, R, fw)
    out, grads, stats = pl.pallas_call(
        kernel,
        out_shape=(
            jax.ShapeDtypeStruct((tok, fw), bf16),
            jax.ShapeDtypeStruct(own, f32),
            jax.ShapeDtypeStruct((8, 128), f32),
        ),
        in_specs=[vm, hbm, hbm, hbm, hbm],
        out_specs=(hbm, hbm, vm),
        scratch_shapes=[
            pltpu.VMEM(own, f32),
            pltpu.VMEM((1, tok), i32),
            pltpu.VMEM((tok, 128), i32),
            pltpu.VMEM((tok, 2 * fw), bf16),
            pltpu.VMEM(base_weight.shape, bf16),
            pltpu.VMEM((NK, GROUP, CHUNK, 2 * fw), bf16),
            pltpu.VMEM((NK, GROUP, CHUNK, 2 * fw), bf16),
            pltpu.VMEM((NK, NZ, 2, R, fw), bf16),
            pltpu.VMEM((3, tok, fw), bf16),
            pltpu.VMEM((3, tok, fw), bf16),
            pltpu.VMEM((tok, fw), f32),
            pltpu.VMEM((NK, 2, GROUP * MOST, NZ * R), f32),
            pltpu.VMEM((NK, NX, 2, GROUP * MOST, NZ * R), f32),
            pltpu.VMEM((NK, GROUP, CHUNK, fw), bf16),
            pltpu.VMEM((NK, GROUP, CHUNK, fw), bf16),
            pltpu.VMEM((NK, NZ, 2, R, fw), bf16),
            pltpu.VMEM((NZ, 2, R, fw), f32),
            pltpu.VMEM((NK, 2, 2, R, fw), bf16),
            pltpu.VMEM((NK, 2, 2, R, fw), bf16),
            pltpu.VMEM((NK, 2, R, fw), bf16),
            pltpu.VMEM((NK, 4, 2, R, fw), bf16),
            pltpu.VMEM(own, f32),
            pltpu.VMEM((tok, fw), bf16),
            pltpu.VMEM((8, 128), f32),
            pltpu.VMEM((NX, 8, 128), f32),
            pltpu.VMEM((8, 128), f32),
            pltpu.VMEM((GROUP, 8, 128), f32),
            pltpu.VMEM((8, 128), f32),
            pltpu.VMEM((NZ, 8, 128), f32),
            dma((4,)), dma((2,)),
            dma((NK, 7)), dma((NK, 7)),
            dma((NK, 8)), dma((NK, 8)),
            dma((NK, 3)), dma((NK, 3)),
            dma((NK, 3)), dma((NK, 3)),
            dma((NK, 7)), dma((NK, 7)),
            dma((NK, 8)), dma((NK, 8)),
            dma((3,)), dma((3,)),
            dma((7,)), dma((7,)),
            dma((7,)), dma((7,)),
        ],
        compiler_params=pltpu.CompilerParams(
            collective_id=0, has_side_effects=True, vmem_limit_bytes=62 * 1024 * 1024
        ),
    )(adapter_ids.reshape(1, tok), inputs, cotangent, base_weight, adapters)
    out, new_adapters, new_first, new_second, norm = pl.pallas_call(
        finish,
        out_shape=(
            jax.ShapeDtypeStruct((tok, fw), bf16),
            jax.ShapeDtypeStruct(own, f32),
            jax.ShapeDtypeStruct(own, f32),
            jax.ShapeDtypeStruct(own, f32),
            jax.ShapeDtypeStruct((1, 1), f32),
        ),
        in_specs=[vm] * 6,
        out_specs=(vm,) * 5,
        compiler_params=pltpu.CompilerParams(vmem_limit_bytes=62 * 1024 * 1024),
    )(out, grads, stats, adapters, first_moment, second_moment)
    return (out, new_adapters, new_first, new_second, norm.reshape(()))


def solution(mesh):
    in_specs = (
        P("aa", "ba"),
        P("aa", "ba"),
        P(None, "ba"),
        P("aa", None),
        P("aa", None, None, "ba"),
        P("aa", None, None, "ba"),
        P("aa", None, None, "ba"),
    )
    out_specs = (
        P("aa", "ba"),
        P("aa", None, None, "ba"),
        P("aa", None, None, "ba"),
        P("aa", None, None, "ba"),
        P(),
    )
    return jax.shard_map(local, mesh=mesh, in_specs=in_specs, out_specs=out_specs, check_vma=False)
```

```python
import math

import jax
import jax.numpy as jnp
from jax import lax
from jax.experimental import pallas as pl
from jax.experimental.pallas import tpu as pltpu
from jax.sharding import PartitionSpec as P

MODEL_WIDTH = 3584
R = 16
NY, NZ, NC, NX = 4, 8, 2, 4
NK = 4
MOST = 4
GROUP = NY * NC
CHUNK = NZ * MOST
MESH = pl.DeviceIdType.MESH

adapter_scale = 2.0
beta_first = 0.9
beta_second = 0.999
adam_eps = 1e-08
learn_rate = 0.01
bias_first = 1.0 - math.exp(1000.0 * math.log(beta_first))
bias_second = 1.0 - math.exp(1000.0 * math.log(beta_second))

EX = ((2, 0), (2, 1), (1, 0), (3, 0), (1, 1), (3, 1), (0, 1))
ZOFF = (4, 3, 5, 2, 6, 1, 7)
XOFF = (2, 1, 3)
ALL = tuple((dy, dc, dx) for dy in (2, 1, 3, 0) for dx in (2, 1, 3, 0) for dc in (1, 0) if (dy, dc, dx) != (0, 0, 0))
f32, bf16, i32 = jnp.float32, jnp.bfloat16, jnp.int32


def nt(a, b):
    return lax.dot_general(a, b, (((1,), (1,)), ((), ())), preferred_element_type=f32)


def nn(a, b):
    return jnp.dot(a, b, preferred_element_type=f32)


def kernel(
    ids_hbm, x_hbm, g_hbm, w_hbm, ad_hbm,
    out_hbm, grad_hbm, st_ref,
    adf, ids, posr, posc, xg, w, snd, rcv, adb, far, via, bs, br, acc, cs, cr, ls, lr, gs, gf, hs, hr, gr, gown, obf,
    sqs, sqr, ts, ty, us, tz,
    lsem, osem, ex_s, ex_r, ag_s, ag_r, f_s, f_r, b_s, b_r, c_s, c_r, l_s, l_r, g_s, g_r, h_r, q_s, q_r, y_s, y_r, z_s, z_r,
):
    a = lax.axis_index("aa")
    x = lax.axis_index("ba")
    y, z, c = a // (NZ * NC), (a // NC) % NZ, a % NC
    me = y * NC + c
    tok, fw = x_hbm.shape
    nrow = GROUP * CHUNK
    quarter = tok // NK

    def at_yc(dy, dc):
        yy, cc = (y + dy) % NY, (c + dc) % NC
        return yy * NC + cc, ((yy * NZ + z) * NC + cc, x)

    def at_z(dz):
        zz = (z + dz + NZ) % NZ
        return zz, ((y * NZ + zz) * NC + c, x)

    def at_all(dy, dc, dx):
        yy, cc = (y + dy) % NY, (c + dc) % NC
        return (yy * NZ + z) * NC + cc, (x + dx) % NX

    def at_x(dx):
        xx = (x + dx) % NX
        return xx, (a, xx)

    barrier = pltpu.get_barrier_semaphore()
    for dz in ZOFF:
        pl.semaphore_signal(barrier, inc=1, device_id=at_z(dz)[1], device_id_type=MESH)
    for step in ALL:
        pl.semaphore_signal(barrier, inc=1, device_id=at_all(*step), device_id_type=MESH)

    loads = [
        pltpu.make_async_copy(ad_hbm, adf, lsem.at[0]),
        pltpu.make_async_copy(ids_hbm, ids, lsem.at[4]),
        pltpu.make_async_copy(x_hbm, xg.at[:, 0:fw], lsem.at[1]),
        pltpu.make_async_copy(g_hbm, xg.at[:, fw : 2 * fw], lsem.at[2]),
        pltpu.make_async_copy(w_hbm, w, lsem.at[3]),
    ]
    for cp in loads:
        cp.start()

    def remote(src, dst, ssem, rsem, dev):
        return pltpu.make_async_remote_copy(
            src_ref=src, dst_ref=dst, send_sem=ssem, recv_sem=rsem, device_id=dev, device_id_type=MESH
        )

    def arrived(ref, sem):
        remote(ref, ref, sem, sem, at_x(1)[1]).wait_recv()

    def left(ref, sem):
        remote(ref, ref, sem, sem, at_x(1)[1]).wait_send()

    def ex_copy(k, j):
        d, dev = at_yc(*EX[j])
        return remote(snd.at[k, d], rcv.at[k, me], ex_s, ex_r.at[k], dev)

    def lora_copy(k, j):
        d, dev = at_yc(*EX[j])
        return remote(ls.at[k, d], lr.at[k, me], l_s, l_r.at[k], dev)

    def ag_copy(k, s, up):
        o, i = at_z(-s if up else s)[0], s if up else 4 + s
        return remote(adb.at[k, o], adb.at[k, o], ag_s, ag_r.at[k, i], at_z(1 if up else -1)[1])

    def g_copy(k, j):
        side = 1 if j % 2 == 0 else -1
        if j < 2:
            src, dst, to, sem = gs.at[k, at_z(side)[0]], gr.at[k, j], side, g_r.at[k]
        elif j < 4:
            src, dst, to, sem = gs.at[k, at_z(3 * side)[0]], hr.at[k, j - 2, 0:2], side, h_r.at[k, j - 2]
        elif j < 6:
            src, dst, to, sem = gs.at[k, at_z(4)[0], j - 4], hr.at[k, j - 4, 2], 2 * side, h_r.at[k, j - 4]
        else:
            src, dst, to, sem = hs.at[k, j - 6], gr.at[k, j - 4], 2 * side, g_r.at[k]
        return remote(src, dst, g_s, sem, at_z(to)[1])

    def far_copy(j):
        half = pl.ds(j * (tok // 2), tok // 2)
        return remote(far.at[half, :], via.at[j], f_s, f_r.at[j], at_x(1 if j == 0 else 3)[1])

    def near_copy(q, j):
        here = pl.ds(q * quarter, quarter)
        return remote(bs.at[j, here, :], br.at[j, here, :], b_s, b_r.at[q], at_x(1 if j == 0 else 3)[1])

    def c_copy(k, j):
        return remote(cs.at[k], cr.at[k, x], c_s, c_r.at[k], at_x(XOFF[j])[1])

    def q_copy(j):
        return remote(sqs, sqr.at[x], q_s, q_r, at_x(XOFF[j])[1])

    def y_copy(j):
        return remote(us, ty.at[x * GROUP + me], y_s, y_r, at_all(*ALL[j]))

    def z_copy(j):
        return remote(ts, tz.at[z], z_s, z_r, at_z(ZOFF[j])[1])

    def positions():
        row = ids[...]
        col = jnp.broadcast_to(row, (128, tok)).T[:, 0:1]
        before = lax.broadcasted_iota(i32, (tok, 1), 0) < lax.broadcasted_iota(i32, (1, tok), 1)
        rank = jnp.sum(jnp.where((col == row) & before, 1, 0), axis=0, keepdims=True)
        k, core = row & (NK - 1), (row >> 2) & (NC - 1)
        zz, yy = (row >> 3) & (NZ - 1), row >> 6
        pos = ((k * GROUP + yy * NC + core) * MOST + rank) * NZ + zz
        posr[...] = pos
        posc[...] = jnp.broadcast_to(pos, (128, tok)).T

    def gather(k):
        rows = lax.broadcasted_iota(i32, (nrow, 1), 0) + k * nrow
        hot = jnp.where(rows == posr[...], 1.0, 0.0).astype(bf16)
        snd[k] = nn(hot, xg[...]).astype(bf16).reshape(GROUP, CHUNK, 2 * fw)
        rcv[k, me] = snd[k, me]

    def send_tokens(k):
        for j in range(len(EX)):
            ex_copy(k, j).start()

    def frozen_of(dx, here):
        xx = at_x(dx)[0]
        return nt(xg[here, fw : 2 * fw], w[pl.ds(pl.multiple_of(xx * fw, fw), fw), :])

    def frozen_far():
        far[...] = frozen_of(2, slice(None)).astype(bf16)
        for j in range(2):
            far_copy(j).start()

    def frozen_near(q):
        here = pl.ds(q * quarter, quarter)
        for j in range(2):
            t = frozen_of(1 if j == 0 else 3, here)
            if q // 2 == j:
                if q % 2 == 0:
                    arrived(via.at[j], f_r.at[j])
                t = t + via[j, pl.ds((q % 2) * quarter, quarter), :].astype(f32)
            bs[j, here, :] = t.astype(bf16)
            near_copy(q, j).start()

    def ag_ways(k, s):
        return [up for up in (True, False) if s < 3 or up == (k % 2 == 0)]

    def ag_pass(k, s):
        for up in ag_ways(k, s):
            if s > 0:
                ag_copy(k, s - 1, up).wait_recv()
            ag_copy(k, s, up).start()

    def ag_end(k):
        for up in (True, False):
            ag_copy(k, 3 if up in ag_ways(k, 3) else 2, up).wait_recv()

    lane = lax.broadcasted_iota(i32, (1, NZ, NZ * R), 2) // R
    sub = lax.broadcasted_iota(i32, (1, NZ, NZ * R), 1)
    mine = lane == sub

    def rows_of(k, first):
        return rcv[k, :, :, first : first + fw].reshape(nrow, fw)

    def project(k):
        pulled = nt(rows_of(k, fw), adb[k, :, 1].reshape(NZ * R, fw)).reshape(GROUP * MOST, NZ, NZ * R)
        projected = nt(rows_of(k, 0), adb[k, :, 0].reshape(NZ * R, fw)).reshape(GROUP * MOST, NZ, NZ * R)
        cs[k, 0] = jnp.sum(jnp.where(mine, pulled, 0.0), axis=1)
        cs[k, 1] = jnp.sum(jnp.where(mine, projected, 0.0), axis=1)
        cr[k, x] = cs[k]
        for j in range(len(XOFF)):
            c_copy(k, j).start()

    def gradients(k):
        low = (cr[k, 0] + cr[k, 1] + cr[k, 2] + cr[k, 3]).astype(bf16).astype(f32)
        pull = jnp.where(mine, low[0][:, None, :], 0.0).reshape(nrow, NZ * R)
        proj = jnp.where(mine, low[1][:, None, :], 0.0).reshape(nrow, NZ * R)
        for i, (side, first) in enumerate(((pull, 0), (proj, fw))):
            grad = (adapter_scale * nn(side.T.astype(bf16), rows_of(k, first))).reshape(NZ, R, fw)
            gf[:, i] = grad
            gs[k, :, i] = grad.astype(bf16)
        for j in (2, 3, 4, 5, 0, 1):
            g_copy(k, j).start()
        gown[k] = gf[z]
        lora = adapter_scale * nn(pull.astype(bf16), adb[k, :, 0].reshape(NZ * R, fw))
        ls[k] = lora.astype(bf16).reshape(GROUP, CHUNK, fw)
        for j in range(len(EX)):
            lora_copy(k, j).start()
        lr[k, me] = ls[k, me]

    def hub(k):
        for side in range(2):
            arrived(hr.at[k, side], h_r.at[k, side])
            sign = 1 if side == 0 else -1
            for i in range(2):
                t = gf[at_z(2 * sign)[0], i] + hr[k, side, i].astype(f32)
                if i == side:
                    t = t + hr[k, side, 2].astype(f32)
                hs[k, side, i] = t.astype(bf16)
            g_copy(k, 6 + side).start()

    def unslot(k):
        cols = lax.broadcasted_iota(i32, (1, nrow), 1) + k * nrow
        hot = jnp.where(posc[:, 0:1] == cols, 1.0, 0.0).astype(bf16)
        acc[...] += nn(hot, lr[k].reshape(nrow, fw))

    def total_gradient(k):
        arrived(gr.at[k], g_r.at[k])
        t = gown[k]
        for j in range(4):
            t = t + gr[k, j].astype(f32)
        gown[k] = t
        return jnp.sum(t * t)

    loads[0].wait()
    for k in range(2):
        adb[k, z] = adf[k].astype(bf16)
    for cp in loads[1:4]:
        cp.wait()
    positions()
    gather(0)
    pl.semaphore_wait(barrier, len(ZOFF) + len(ALL))
    ag_pass(0, 0)
    send_tokens(0)
    ag_pass(1, 0)
    for k in range(2, NK):
        adb[k, z] = adf[k].astype(bf16)
    loads[4].wait()
    frozen_far()
    ag_pass(0, 1)
    ag_pass(2, 0)
    gather(1)
    send_tokens(1)
    ag_pass(1, 1)
    ag_pass(3, 0)
    gather(2)
    send_tokens(2)
    ag_pass(0, 2)
    ag_pass(2, 1)
    gather(3)
    send_tokens(3)
    ag_pass(1, 2)
    ag_pass(3, 1)
    acc[...] = frozen_of(0, slice(None))
    ag_pass(0, 3)
    ag_pass(2, 2)
    ag_pass(1, 3)
    ag_end(0)

    for k in range(NK):
        if k == NK - 1:
            hub(k - 1)
        if k > 0:
            ag_end(k)
        arrived(rcv.at[k, 0 : GROUP - 1], ex_r.at[k])
        project(k)
        if k == 0:
            ag_pass(3, 2)
            ag_pass(2, 3)
            ag_pass(3, 3)
        elif k < NK - 1:
            hub(k - 1)
        arrived(cr.at[k, 0 : NX - 1], c_r.at[k])
        gradients(k)
        frozen_near(k)

    def frozen(q):
        here = pl.ds(q * quarter, quarter)
        arrived(br.at[:, here, :], b_r.at[q])
        t = acc[here, :]
        for j in range(2):
            t = t + br[j, here, :].astype(f32)
        acc[here, :] = t

    def lora_wait(k):
        arrived(lr.at[k, 0 : GROUP - 1], l_r.at[k])

    frozen(0)
    frozen(1)
    lora_wait(0)
    unslot(0)
    hub(NK - 1)
    frozen(2)
    lora_wait(1)
    unslot(1)
    row = lax.broadcasted_iota(i32, (8, 128), 0)
    sq = jnp.zeros((8, 128), f32)
    for k in range(NK):
        sq = sq + jnp.where(row == k, total_gradient(k), 0.0)
    sqs[...] = sq
    ts[...] = jnp.sum(sq, axis=0, keepdims=True)
    for j in range(len(ZOFF)):
        z_copy(j).start()
    for j in range(len(XOFF)):
        q_copy(j).start()
    sqr[x] = sq
    tz[z] = ts[...]
    grad_out = pltpu.make_async_copy(gown, grad_hbm, osem.at[0])
    grad_out.start()
    frozen(3)
    arrived(tz.at[0 : NZ - 1], z_r)
    us[...] = jnp.sum(tz[...], axis=0)
    for j in range(len(ALL)):
        y_copy(j).start()
    ty[x * GROUP + me] = us[...]
    lora_wait(2)
    unslot(2)
    arrived(sqr.at[0 : NX - 1], q_r)
    squares = sqr[0] + sqr[1] + sqr[2] + sqr[3]
    lora_wait(3)
    unslot(3)
    obf[...] = acc[...].astype(bf16)
    out_copy = pltpu.make_async_copy(obf, out_hbm, osem.at[1])
    out_copy.start()
    left(snd.at[:, 0 : GROUP - 1], ex_s)
    left(ls.at[:, 0 : GROUP - 1], l_s)
    left(adb.at[:, 0 : NZ - 1], ag_s)
    left(gs.at[:, 0 : NZ - 1], g_s)
    left(bs, b_s)
    left(far, f_s)
    left(cr.at[:, 0 : NX - 1], c_s)
    left(sqr.at[0 : NX - 1], q_s)
    left(tz.at[0 : NZ - 1], z_s)
    grad_out.wait()
    arrived(ty.at[0 : len(ALL)], y_r)
    st_ref[...] = jnp.where(row == NK, jnp.sum(ty[...], axis=0), squares)
    left(ty.at[0 : len(ALL)], y_s)
    out_copy.wait()


def finish(out_ref, grad_ref, st_ref, ad_ref, m_ref, v_ref, o_ref, na_ref, nf_ref, ns_ref, norm_ref):
    clip_limit = math.sqrt(2.0 * R * MODEL_WIDTH)
    o_ref[...] = out_ref[...]
    for k in range(NK):
        factor = clip_limit / jnp.maximum(jnp.sqrt(st_ref[k : k + 1, 0:1]), clip_limit)
        clipped = grad_ref[k] * factor
        new_first = beta_first * m_ref[k] + (1.0 - beta_first) * clipped
        new_second = beta_second * v_ref[k] + (1.0 - beta_second) * clipped * clipped
        update = new_first / bias_first / (jnp.sqrt(new_second / bias_second) + adam_eps)
        na_ref[k] = ad_ref[k] - learn_rate * update
        nf_ref[k] = new_first
        ns_ref[k] = new_second
    norm_ref[...] = jnp.sqrt(st_ref[NK : NK + 1, 0:1])


def local(inputs, cotangent, base_weight, adapter_ids, adapters, first_moment, second_moment):
    tok, fw = inputs.shape
    dma = pltpu.SemaphoreType.DMA
    vm, hbm = pl.BlockSpec(memory_space=pltpu.VMEM), pl.BlockSpec(memory_space=pl.ANY)
    own = (NK, 2, R, fw)
    out, grads, stats = pl.pallas_call(
        kernel,
        out_shape=(
            jax.ShapeDtypeStruct((tok, fw), bf16),
            jax.ShapeDtypeStruct(own, f32),
            jax.ShapeDtypeStruct((8, 128), f32),
        ),
        in_specs=[hbm] * 5,
        out_specs=(hbm, hbm, vm),
        scratch_shapes=[
            pltpu.VMEM(own, f32),
            pltpu.VMEM((1, tok), i32),
            pltpu.VMEM((1, tok), i32),
            pltpu.VMEM((tok, 128), i32),
            pltpu.VMEM((tok, 2 * fw), bf16),
            pltpu.VMEM(base_weight.shape, bf16),
            pltpu.VMEM((NK, GROUP, CHUNK, 2 * fw), bf16),
            pltpu.VMEM((NK, GROUP, CHUNK, 2 * fw), bf16),
            pltpu.VMEM((NK, NZ, 2, R, fw), bf16),
            pltpu.VMEM((tok, fw), bf16),
            pltpu.VMEM((2, tok // 2, fw), bf16),
            pltpu.VMEM((2, tok, fw), bf16),
            pltpu.VMEM((2, tok, fw), bf16),
            pltpu.VMEM((tok, fw), f32),
            pltpu.VMEM((NK, 2, GROUP * MOST, NZ * R), f32),
            pltpu.VMEM((NK, NX, 2, GROUP * MOST, NZ * R), f32),
            pltpu.VMEM((NK, GROUP, CHUNK, fw), bf16),
            pltpu.VMEM((NK, GROUP, CHUNK, fw), bf16),
            pltpu.VMEM((NK, NZ, 2, R, fw), bf16),
            pltpu.VMEM((NZ, 2, R, fw), f32),
            pltpu.VMEM((NK, 2, 2, R, fw), bf16),
            pltpu.VMEM((NK, 2, 3, R, fw), bf16),
            pltpu.VMEM((NK, 4, 2, R, fw), bf16),
            pltpu.VMEM(own, f32),
            pltpu.VMEM((tok, fw), bf16),
            pltpu.VMEM((8, 128), f32),
            pltpu.VMEM((NX, 8, 128), f32),
            pltpu.VMEM((1, 128), f32),
            pltpu.VMEM((NX * GROUP, 1, 128), f32),
            pltpu.VMEM((1, 128), f32),
            pltpu.VMEM((NZ, 1, 128), f32),
            dma((5,)), dma((2,)),
            dma, dma((NK,)),
            dma, dma((NK, 8)),
            dma, dma((2,)),
            dma, dma((NK,)),
            dma, dma((NK,)),
            dma, dma((NK,)),
            dma, dma((NK,)), dma((NK, 2)),
            dma, dma,
            dma, dma,
            dma, dma,
        ],
        compiler_params=pltpu.CompilerParams(
            collective_id=0, has_side_effects=True, vmem_limit_bytes=62 * 1024 * 1024
        ),
    )(adapter_ids.reshape(1, tok), inputs, cotangent, base_weight, adapters)
    out, new_adapters, new_first, new_second, norm = pl.pallas_call(
        finish,
        out_shape=(
            jax.ShapeDtypeStruct((tok, fw), bf16),
            jax.ShapeDtypeStruct(own, f32),
            jax.ShapeDtypeStruct(own, f32),
            jax.ShapeDtypeStruct(own, f32),
            jax.ShapeDtypeStruct((1, 1), f32),
        ),
        in_specs=[vm] * 6,
        out_specs=(vm,) * 5,
        compiler_params=pltpu.CompilerParams(vmem_limit_bytes=62 * 1024 * 1024),
    )(out, grads, stats, adapters, first_moment, second_moment)
    return (out, new_adapters, new_first, new_second, norm.reshape(()))


def solution(mesh):
    in_specs = (
        P("aa", "ba"),
        P("aa", "ba"),
        P(None, "ba"),
        P("aa", None),
        P("aa", None, None, "ba"),
        P("aa", None, None, "ba"),
        P("aa", None, None, "ba"),
    )
    out_specs = (
        P("aa", "ba"),
        P("aa", None, None, "ba"),
        P("aa", None, None, "ba"),
        P("aa", None, None, "ba"),
        P(),
    )
    return jax.shard_map(local, mesh=mesh, in_specs=in_specs, out_specs=out_specs, check_vma=False)
```

```python
import math

import jax
import jax.numpy as jnp
from jax import lax
from jax.experimental import pallas as pl
from jax.experimental.pallas import tpu as pltpu
from jax.sharding import PartitionSpec as P

MODEL_WIDTH = 3584
R = 16
NY, NZ, NC, NX = 4, 8, 2, 4
NK = 4
MOST = 4
GROUP = NY * NC
CHUNK = NZ * MOST
MESH = pl.DeviceIdType.MESH

adapter_scale = 2.0
beta_first = 0.9
beta_second = 0.999
adam_eps = 1e-08
learn_rate = 0.01
clip_limit = math.sqrt(2.0 * R * MODEL_WIDTH)
bias_first = 1.0 - math.exp(1000.0 * math.log(beta_first))
bias_second = 1.0 - math.exp(1000.0 * math.log(beta_second))

EX = ((2, 0), (2, 1), (1, 0), (3, 0), (1, 1), (3, 1), (0, 1))
ZOFF = (4, 3, 5, 2, 6, 1, 7)
XOFF = (2, 1, 3)
ALL = tuple((dy, dc, dx) for dy in (2, 1, 3, 0) for dx in (2, 1, 3, 0) for dc in (1, 0) if (dy, dc, dx) != (0, 0, 0))
f32, bf16, i32 = jnp.float32, jnp.bfloat16, jnp.int32


def nt(a, b):
    return lax.dot_general(a, b, (((1,), (1,)), ((), ())), preferred_element_type=f32)


def nn(a, b):
    return jnp.dot(a, b, preferred_element_type=f32)


def kernel(
    ids_hbm, x_hbm, g_hbm, w_hbm, ad_hbm, m_hbm, v_hbm,
    out_hbm, na_hbm, nf_hbm, ns_hbm, st_ref,
    adf, mb, vb, ids, posr, posc, xg, w, snd, rcv, adb, far, via, bs, br, acc, cs, cr, ls, lr, gs, gf, hs, hr, gr, gown, obf,
    sqs, sqr, ts, ty, us, tz,
    lsem, osem, ex_s, ex_r, ag_s, ag_r, f_s, f_r, b_s, b_r, c_s, c_r, l_s, l_r, g_s, g_r, h_r, q_s, q_r, y_s, y_r, z_s, z_r,
):
    a = lax.axis_index("aa")
    x = lax.axis_index("ba")
    y, z, c = a // (NZ * NC), (a // NC) % NZ, a % NC
    me = y * NC + c
    tok, fw = x_hbm.shape
    nrow = GROUP * CHUNK
    quarter = tok // NK

    def at_yc(dy, dc):
        yy, cc = (y + dy) % NY, (c + dc) % NC
        return yy * NC + cc, ((yy * NZ + z) * NC + cc, x)

    def at_z(dz):
        zz = (z + dz + NZ) % NZ
        return zz, ((y * NZ + zz) * NC + c, x)

    def at_all(dy, dc, dx):
        yy, cc = (y + dy) % NY, (c + dc) % NC
        return (yy * NZ + z) * NC + cc, (x + dx) % NX

    def at_x(dx):
        xx = (x + dx) % NX
        return xx, (a, xx)

    barrier = pltpu.get_barrier_semaphore()
    for dz in ZOFF:
        pl.semaphore_signal(barrier, inc=1, device_id=at_z(dz)[1], device_id_type=MESH)
    for step in ALL:
        pl.semaphore_signal(barrier, inc=1, device_id=at_all(*step), device_id_type=MESH)

    loads = [
        pltpu.make_async_copy(ad_hbm, adf, lsem.at[0]),
        pltpu.make_async_copy(ids_hbm, ids, lsem.at[4]),
        pltpu.make_async_copy(x_hbm, xg.at[:, 0:fw], lsem.at[1]),
        pltpu.make_async_copy(g_hbm, xg.at[:, fw : 2 * fw], lsem.at[2]),
        pltpu.make_async_copy(w_hbm, w, lsem.at[3]),
        pltpu.make_async_copy(m_hbm, mb, lsem.at[5]),
        pltpu.make_async_copy(v_hbm, vb, lsem.at[6]),
    ]
    for cp in loads:
        cp.start()

    def remote(src, dst, ssem, rsem, dev):
        return pltpu.make_async_remote_copy(
            src_ref=src, dst_ref=dst, send_sem=ssem, recv_sem=rsem, device_id=dev, device_id_type=MESH
        )

    def arrived(ref, sem):
        remote(ref, ref, sem, sem, at_x(1)[1]).wait_recv()

    def left(ref, sem):
        remote(ref, ref, sem, sem, at_x(1)[1]).wait_send()

    def ex_copy(k, j):
        d, dev = at_yc(*EX[j])
        return remote(snd.at[k, d], rcv.at[k, me], ex_s, ex_r.at[k], dev)

    def lora_copy(k, j):
        d, dev = at_yc(*EX[j])
        return remote(ls.at[k, d], lr.at[k, me], l_s, l_r.at[k], dev)

    def ag_copy(k, s, up):
        o, i = at_z(-s if up else s)[0], s if up else 4 + s
        return remote(adb.at[k, o], adb.at[k, o], ag_s, ag_r.at[k, i], at_z(1 if up else -1)[1])

    def g_copy(k, j):
        side = 1 if j % 2 == 0 else -1
        if j < 2:
            src, dst, to, sem = gs.at[k, at_z(side)[0]], gr.at[k, j], side, g_r.at[k]
        elif j < 4:
            src, dst, to, sem = gs.at[k, at_z(3 * side)[0]], hr.at[k, j - 2, 0:2], side, h_r.at[k, j - 2]
        elif j < 6:
            src, dst, to, sem = gs.at[k, at_z(4)[0], j - 4], hr.at[k, j - 4, 2], 2 * side, h_r.at[k, j - 4]
        else:
            src, dst, to, sem = hs.at[k, j - 6], gr.at[k, j - 4], 2 * side, g_r.at[k]
        return remote(src, dst, g_s, sem, at_z(to)[1])

    def far_copy(j):
        half = pl.ds(j * (tok // 2), tok // 2)
        return remote(far.at[half, :], via.at[j], f_s, f_r.at[j], at_x(1 if j == 0 else 3)[1])

    def near_copy(q, j):
        here = pl.ds(q * quarter, quarter)
        return remote(bs.at[j, here, :], br.at[j, here, :], b_s, b_r.at[q], at_x(1 if j == 0 else 3)[1])

    def c_copy(k, j):
        return remote(cs.at[k], cr.at[k, x], c_s, c_r.at[k], at_x(XOFF[j])[1])

    def q_copy(j):
        return remote(sqs, sqr.at[x], q_s, q_r, at_x(XOFF[j])[1])

    def y_copy(j):
        return remote(us, ty.at[x * GROUP + me], y_s, y_r, at_all(*ALL[j]))

    def z_copy(j):
        return remote(ts, tz.at[z], z_s, z_r, at_z(ZOFF[j])[1])

    def positions():
        row = ids[...]
        col = jnp.broadcast_to(row, (128, tok)).T[:, 0:1]
        before = lax.broadcasted_iota(i32, (tok, 1), 0) < lax.broadcasted_iota(i32, (1, tok), 1)
        rank = jnp.sum(jnp.where((col == row) & before, 1, 0), axis=0, keepdims=True)
        k, core = row & (NK - 1), (row >> 2) & (NC - 1)
        zz, yy = (row >> 3) & (NZ - 1), row >> 6
        pos = ((k * GROUP + yy * NC + core) * MOST + rank) * NZ + zz
        posr[...] = pos
        posc[...] = jnp.broadcast_to(pos, (128, tok)).T

    def gather(k):
        rows = lax.broadcasted_iota(i32, (nrow, 1), 0) + k * nrow
        hot = jnp.where(rows == posr[...], 1.0, 0.0).astype(bf16)
        snd[k] = nn(hot, xg[...]).astype(bf16).reshape(GROUP, CHUNK, 2 * fw)
        rcv[k, me] = snd[k, me]

    def send_tokens(k):
        for j in range(len(EX)):
            ex_copy(k, j).start()

    def frozen_of(dx, here):
        xx = at_x(dx)[0]
        return nt(xg[here, fw : 2 * fw], w[pl.ds(pl.multiple_of(xx * fw, fw), fw), :])

    def frozen_far():
        far[...] = frozen_of(2, slice(None)).astype(bf16)
        for j in range(2):
            far_copy(j).start()

    def frozen_near(q):
        here = pl.ds(q * quarter, quarter)
        for j in range(2):
            t = frozen_of(1 if j == 0 else 3, here)
            if q // 2 == j:
                if q % 2 == 0:
                    arrived(via.at[j], f_r.at[j])
                t = t + via[j, pl.ds((q % 2) * quarter, quarter), :].astype(f32)
            bs[j, here, :] = t.astype(bf16)
            near_copy(q, j).start()

    def ag_ways(k, s):
        return [up for up in (True, False) if s < 3 or up == (k % 2 == 0)]

    def ag_pass(k, s):
        for up in ag_ways(k, s):
            if s > 0:
                ag_copy(k, s - 1, up).wait_recv()
            ag_copy(k, s, up).start()

    def ag_end(k):
        for up in (True, False):
            ag_copy(k, 3 if up in ag_ways(k, 3) else 2, up).wait_recv()

    lane = lax.broadcasted_iota(i32, (1, NZ, NZ * R), 2) // R
    sub = lax.broadcasted_iota(i32, (1, NZ, NZ * R), 1)
    mine = lane == sub

    def rows_of(k, first):
        return rcv[k, :, :, first : first + fw].reshape(nrow, fw)

    def project(k):
        pulled = nt(rows_of(k, fw), adb[k, :, 1].reshape(NZ * R, fw)).reshape(GROUP * MOST, NZ, NZ * R)
        projected = nt(rows_of(k, 0), adb[k, :, 0].reshape(NZ * R, fw)).reshape(GROUP * MOST, NZ, NZ * R)
        cs[k, 0] = jnp.sum(jnp.where(mine, pulled, 0.0), axis=1)
        cs[k, 1] = jnp.sum(jnp.where(mine, projected, 0.0), axis=1)
        cr[k, x] = cs[k]
        for j in range(len(XOFF)):
            c_copy(k, j).start()

    def gradients(k):
        low = (cr[k, 0] + cr[k, 1] + cr[k, 2] + cr[k, 3]).astype(bf16).astype(f32)
        pull = jnp.where(mine, low[0][:, None, :], 0.0).reshape(nrow, NZ * R)
        proj = jnp.where(mine, low[1][:, None, :], 0.0).reshape(nrow, NZ * R)
        for i, (side, first) in enumerate(((pull, 0), (proj, fw))):
            grad = (adapter_scale * nn(side.T.astype(bf16), rows_of(k, first))).reshape(NZ, R, fw)
            gf[:, i] = grad
            gs[k, :, i] = grad.astype(bf16)
        for j in (2, 3, 4, 5, 0, 1):
            g_copy(k, j).start()
        gown[k] = gf[z]
        lora = adapter_scale * nn(pull.astype(bf16), adb[k, :, 0].reshape(NZ * R, fw))
        ls[k] = lora.astype(bf16).reshape(GROUP, CHUNK, fw)
        for j in range(len(EX)):
            lora_copy(k, j).start()
        lr[k, me] = ls[k, me]

    def hub(k):
        for side in range(2):
            arrived(hr.at[k, side], h_r.at[k, side])
            sign = 1 if side == 0 else -1
            for i in range(2):
                t = gf[at_z(2 * sign)[0], i] + hr[k, side, i].astype(f32)
                if i == side:
                    t = t + hr[k, side, 2].astype(f32)
                hs[k, side, i] = t.astype(bf16)
            g_copy(k, 6 + side).start()

    def unslot(k):
        cols = lax.broadcasted_iota(i32, (1, nrow), 1) + k * nrow
        hot = jnp.where(posc[:, 0:1] == cols, 1.0, 0.0).astype(bf16)
        acc[...] += nn(hot, lr[k].reshape(nrow, fw))

    def total_gradient(k):
        arrived(gr.at[k], g_r.at[k])
        t = gown[k]
        for j in range(4):
            t = t + gr[k, j].astype(f32)
        gown[k] = t
        return jnp.sum(t * t)

    loads[0].wait()
    for k in range(2):
        adb[k, z] = adf[k].astype(bf16)
    for cp in loads[1:4]:
        cp.wait()
    positions()
    gather(0)
    pl.semaphore_wait(barrier, len(ZOFF) + len(ALL))
    ag_pass(0, 0)
    send_tokens(0)
    ag_pass(1, 0)
    for k in range(2, NK):
        adb[k, z] = adf[k].astype(bf16)
    for cp in loads[4:]:
        cp.wait()
    frozen_far()
    ag_pass(0, 1)
    ag_pass(2, 0)
    gather(1)
    send_tokens(1)
    ag_pass(1, 1)
    ag_pass(3, 0)
    gather(2)
    send_tokens(2)
    ag_pass(0, 2)
    ag_pass(2, 1)
    gather(3)
    send_tokens(3)
    ag_pass(1, 2)
    ag_pass(3, 1)
    acc[...] = frozen_of(0, slice(None))
    ag_pass(0, 3)
    frozen_near(0)
    ag_pass(2, 2)
    ag_pass(1, 3)
    ag_end(0)

    for k in range(NK):
        if k == NK - 1:
            hub(k - 1)
        if k > 0:
            ag_end(k)
        arrived(rcv.at[k, 0 : GROUP - 1], ex_r.at[k])
        project(k)
        if k + 1 < NK:
            frozen_near(k + 1)
        if k == 0:
            ag_pass(3, 2)
            ag_pass(2, 3)
            ag_pass(3, 3)
        elif k < NK - 1:
            hub(k - 1)
        arrived(cr.at[k, 0 : NX - 1], c_r.at[k])
        gradients(k)

    def frozen(q):
        here = pl.ds(q * quarter, quarter)
        arrived(br.at[:, here, :], b_r.at[q])
        t = acc[here, :]
        for j in range(2):
            t = t + br[j, here, :].astype(f32)
        acc[here, :] = t

    def lora_wait(k):
        arrived(lr.at[k, 0 : GROUP - 1], l_r.at[k])

    frozen(0)
    frozen(1)
    lora_wait(0)
    unslot(0)
    hub(NK - 1)
    frozen(2)
    lora_wait(1)
    unslot(1)
    row = lax.broadcasted_iota(i32, (8, 128), 0)
    sq = jnp.zeros((8, 128), f32)
    for k in range(NK):
        sq = sq + jnp.where(row == k, total_gradient(k), 0.0)
    sqs[...] = sq
    ts[...] = jnp.sum(sq, axis=0, keepdims=True)
    for j in range(len(ZOFF)):
        z_copy(j).start()
    for j in range(len(XOFF)):
        q_copy(j).start()
    sqr[x] = sq
    tz[z] = ts[...]
    frozen(3)
    arrived(tz.at[0 : NZ - 1], z_r)
    us[...] = jnp.sum(tz[...], axis=0)
    for j in range(len(ALL)):
        y_copy(j).start()
    ty[x * GROUP + me] = us[...]
    lora_wait(2)
    unslot(2)
    arrived(sqr.at[0 : NX - 1], q_r)
    squares = sqr[0] + sqr[1] + sqr[2] + sqr[3]
    for k in range(NK):
        factor = clip_limit / jnp.maximum(jnp.sqrt(squares[k : k + 1, 0:1]), clip_limit)
        clipped = gown[k] * factor
        new_first = beta_first * mb[k] + (1.0 - beta_first) * clipped
        new_second = beta_second * vb[k] + (1.0 - beta_second) * clipped * clipped
        update = new_first / bias_first / (jnp.sqrt(new_second / bias_second) + adam_eps)
        adf[k] = adf[k] - learn_rate * update
        mb[k] = new_first
        vb[k] = new_second
    moved = [
        pltpu.make_async_copy(src, dst, osem.at[i + 1])
        for i, (src, dst) in enumerate(((adf, na_hbm), (mb, nf_hbm), (vb, ns_hbm)))
    ]
    for cp in moved:
        cp.start()
    lora_wait(3)
    unslot(3)
    obf[...] = acc[...].astype(bf16)
    out_copy = pltpu.make_async_copy(obf, out_hbm, osem.at[0])
    out_copy.start()
    left(snd.at[:, 0 : GROUP - 1], ex_s)
    left(ls.at[:, 0 : GROUP - 1], l_s)
    left(adb.at[:, 0 : NZ - 1], ag_s)
    left(gs.at[:, 0 : NZ - 1], g_s)
    left(bs, b_s)
    left(far, f_s)
    left(cr.at[:, 0 : NX - 1], c_s)
    left(sqr.at[0 : NX - 1], q_s)
    left(tz.at[0 : NZ - 1], z_s)
    arrived(ty.at[0 : len(ALL)], y_r)
    st_ref[...] = jnp.sum(ty[...], axis=0)
    left(ty.at[0 : len(ALL)], y_s)
    for cp in (out_copy, *moved):
        cp.wait()


def finish(o_in, na_in, nf_in, ns_in, st_ref, o_out, na_out, nf_out, ns_out, norm_ref, sem):
    moves = [
        pltpu.make_async_copy(src, dst, sem.at[i])
        for i, (src, dst) in enumerate(((na_in, na_out), (nf_in, nf_out), (ns_in, ns_out), (o_in, o_out)))
    ]
    for cp in moves:
        cp.start()
    norm_ref[...] = jnp.sqrt(st_ref[0:1, 0:1])
    for cp in moves:
        cp.wait()


def local(inputs, cotangent, base_weight, adapter_ids, adapters, first_moment, second_moment):
    tok, fw = inputs.shape
    dma = pltpu.SemaphoreType.DMA
    vm, hbm, anywhere = (pl.BlockSpec(memory_space=m) for m in (pltpu.VMEM, pltpu.HBM, pl.ANY))
    own = (NK, 2, R, fw)
    results = (
        jax.ShapeDtypeStruct((tok, fw), bf16),
        jax.ShapeDtypeStruct(own, f32),
        jax.ShapeDtypeStruct(own, f32),
        jax.ShapeDtypeStruct(own, f32),
    )
    *parts, stats = pl.pallas_call(
        kernel,
        out_shape=(*results, jax.ShapeDtypeStruct((1, 128), f32)),
        in_specs=[hbm] * 7,
        out_specs=(anywhere,) * 4 + (vm,),
        scratch_shapes=[
            pltpu.VMEM(own, f32),
            pltpu.VMEM(own, f32),
            pltpu.VMEM(own, f32),
            pltpu.VMEM((1, tok), i32),
            pltpu.VMEM((1, tok), i32),
            pltpu.VMEM((tok, 128), i32),
            pltpu.VMEM((tok, 2 * fw), bf16),
            pltpu.VMEM(base_weight.shape, bf16),
            pltpu.VMEM((NK, GROUP, CHUNK, 2 * fw), bf16),
            pltpu.VMEM((NK, GROUP, CHUNK, 2 * fw), bf16),
            pltpu.VMEM((NK, NZ, 2, R, fw), bf16),
            pltpu.VMEM((tok, fw), bf16),
            pltpu.VMEM((2, tok // 2, fw), bf16),
            pltpu.VMEM((2, tok, fw), bf16),
            pltpu.VMEM((2, tok, fw), bf16),
            pltpu.VMEM((tok, fw), f32),
            pltpu.VMEM((NK, 2, GROUP * MOST, NZ * R), f32),
            pltpu.VMEM((NK, NX, 2, GROUP * MOST, NZ * R), f32),
            pltpu.VMEM((NK, GROUP, CHUNK, fw), bf16),
            pltpu.VMEM((NK, GROUP, CHUNK, fw), bf16),
            pltpu.VMEM((NK, NZ, 2, R, fw), bf16),
            pltpu.VMEM((NZ, 2, R, fw), f32),
            pltpu.VMEM((NK, 2, 2, R, fw), bf16),
            pltpu.VMEM((NK, 2, 3, R, fw), bf16),
            pltpu.VMEM((NK, 4, 2, R, fw), bf16),
            pltpu.VMEM(own, f32),
            pltpu.VMEM((tok, fw), bf16),
            pltpu.VMEM((8, 128), f32),
            pltpu.VMEM((NX, 8, 128), f32),
            pltpu.VMEM((1, 128), f32),
            pltpu.VMEM((NX * GROUP, 1, 128), f32),
            pltpu.VMEM((1, 128), f32),
            pltpu.VMEM((NZ, 1, 128), f32),
            dma((7,)), dma((4,)),
            dma, dma((NK,)),
            dma, dma((NK, 8)),
            dma, dma((2,)),
            dma, dma((NK,)),
            dma, dma((NK,)),
            dma, dma((NK,)),
            dma, dma((NK,)), dma((NK, 2)),
            dma, dma,
            dma, dma,
            dma, dma,
        ],
        compiler_params=pltpu.CompilerParams(
            collective_id=0, has_side_effects=True, vmem_limit_bytes=46 * 1024 * 1024
        ),
    )(*(pltpu.with_memory_space_constraint(t, pltpu.HBM) for t in (adapter_ids.reshape(1, tok), inputs, cotangent, base_weight, adapters, first_moment, second_moment)))
    out, new_adapters, new_first, new_second, norm = pl.pallas_call(
        finish,
        out_shape=(*results, jax.ShapeDtypeStruct((1, 1), f32)),
        in_specs=[anywhere] * 4 + [vm],
        out_specs=(hbm,) * 4 + (vm,),
        scratch_shapes=[dma((4,))],
        compiler_params=pltpu.CompilerParams(vmem_limit_bytes=8 * 1024 * 1024),
    )(*parts, stats)
    return (out, new_adapters, new_first, new_second, norm.reshape(()))


def solution(mesh):
    in_specs = (
        P("aa", "ba"),
        P("aa", "ba"),
        P(None, "ba"),
        P("aa", None),
        P("aa", None, None, "ba"),
        P("aa", None, None, "ba"),
        P("aa", None, None, "ba"),
    )
    out_specs = (
        P("aa", "ba"),
        P("aa", None, None, "ba"),
        P("aa", None, None, "ba"),
        P("aa", None, None, "ba"),
        P(),
    )
    return jax.shard_map(local, mesh=mesh, in_specs=in_specs, out_specs=out_specs, check_vma=False)
```

```python
import math

import jax
import jax.numpy as jnp
from jax import lax
from jax.experimental import pallas as pl
from jax.experimental.pallas import tpu as pltpu
from jax.sharding import PartitionSpec as P

MODEL_WIDTH = 3584
R = 16
NY, NZ, NC, NX = 4, 8, 2, 4
NK = 4
MOST = 4
GROUP = NY * NC
CHUNK = NZ * MOST
MESH = pl.DeviceIdType.MESH

adapter_scale = 2.0
beta_first = 0.9
beta_second = 0.999
adam_eps = 1e-08
learn_rate = 0.01
clip_limit = math.sqrt(2.0 * R * MODEL_WIDTH)
bias_first = 1.0 - math.exp(1000.0 * math.log(beta_first))
bias_second = 1.0 - math.exp(1000.0 * math.log(beta_second))

EX = ((2, 0), (1, 0), (3, 0), (2, 1), (1, 1), (3, 1), (0, None))
ZOFF = (4, 3, 5, 2, 6, 1, 7)
XOFF = (2, 1, 3)
ALL = tuple((dy, dc, dx) for dy in (2, 1, 3, 0) for dx in (2, 1, 3, 0) for dc in (1, 0) if (dy, dc, dx) != (0, 0, 0))
f32, bf16, i32 = jnp.float32, jnp.bfloat16, jnp.int32


def nt(a, b):
    return lax.dot_general(a, b, (((1,), (1,)), ((), ())), preferred_element_type=f32)


def nn(a, b):
    return jnp.dot(a, b, preferred_element_type=f32)


def kernel(
    ids_hbm, x_hbm, g_hbm, w_hbm, ad_hbm, m_hbm, v_hbm,
    out_hbm, na_hbm, nf_hbm, ns_hbm, st_ref,
    adf, mb, vb, ids, posr, posc, xg, w, snd, rcv, adb, far, via, bs, br, acc, cs, cr, ls, lr, gs, gf, hs, hr, gr, gown, obf,
    sqs, sqr, ts, ty, us, tz,
    lsem, osem, ex_s, ex_r, ag_s, ag_r, f_s, f_r, b_s, b_r, c_s, c_r, l_s, l_r, g_s, g_r, h_r, q_s, q_r, y_s, y_r, z_s, z_r,
):
    a = lax.axis_index("aa")
    x = lax.axis_index("ba")
    y, z, c = a // (NZ * NC), (a // NC) % NZ, a % NC
    me = y * NC + c
    tok, fw = x_hbm.shape
    nrow = GROUP * CHUNK
    quarter = tok // NK

    def at_yc(dy, core):
        yy, cc = (y + dy) % NY, 1 - c if core is None else core
        return yy * NC + cc, ((yy * NZ + z) * NC + cc, x)

    def at_z(dz):
        zz = (z + dz + NZ) % NZ
        return zz, ((y * NZ + zz) * NC + c, x)

    def at_all(dy, dc, dx):
        yy, cc = (y + dy) % NY, (c + dc) % NC
        return (yy * NZ + z) * NC + cc, (x + dx) % NX

    def at_x(dx):
        xx = (x + dx) % NX
        return xx, (a, xx)

    barrier = pltpu.get_barrier_semaphore()
    for dz in ZOFF:
        pl.semaphore_signal(barrier, inc=1, device_id=at_z(dz)[1], device_id_type=MESH)
    for step in ALL:
        pl.semaphore_signal(barrier, inc=1, device_id=at_all(*step), device_id_type=MESH)

    loads = [
        pltpu.make_async_copy(ad_hbm, adf, lsem.at[0]),
        pltpu.make_async_copy(ids_hbm, ids, lsem.at[4]),
        pltpu.make_async_copy(x_hbm, xg.at[:, 0:fw], lsem.at[1]),
        pltpu.make_async_copy(g_hbm, xg.at[:, fw : 2 * fw], lsem.at[2]),
        pltpu.make_async_copy(w_hbm, w, lsem.at[3]),
        pltpu.make_async_copy(m_hbm, mb, lsem.at[5]),
        pltpu.make_async_copy(v_hbm, vb, lsem.at[6]),
    ]
    for cp in loads:
        cp.start()

    def remote(src, dst, ssem, rsem, dev):
        return pltpu.make_async_remote_copy(
            src_ref=src, dst_ref=dst, send_sem=ssem, recv_sem=rsem, device_id=dev, device_id_type=MESH
        )

    def arrived(ref, sem):
        remote(ref, ref, sem, sem, at_x(1)[1]).wait_recv()

    def left(ref, sem):
        remote(ref, ref, sem, sem, at_x(1)[1]).wait_send()

    def ex_copy(k, j):
        d, dev = at_yc(*EX[j])
        return remote(snd.at[k, d], rcv.at[k, me], ex_s, ex_r.at[k], dev)

    def lora_copy(k, j):
        d, dev = at_yc(*EX[j])
        return remote(ls.at[k, d], lr.at[k, me], l_s, l_r.at[k], dev)

    def ag_copy(k, s, up):
        o, i = at_z(-s if up else s)[0], s if up else 4 + s
        return remote(adb.at[k, o], adb.at[k, o], ag_s, ag_r.at[k, i], at_z(1 if up else -1)[1])

    def g_copy(k, j):
        side = 1 if j % 2 == 0 else -1
        if j < 2:
            src, dst, to, sem = gs.at[k, at_z(side)[0]], gr.at[k, j], side, g_r.at[k]
        elif j < 4:
            src, dst, to, sem = gs.at[k, at_z(3 * side)[0]], hr.at[k, j - 2, 0:2], side, h_r.at[k, j - 2]
        elif j < 6:
            src, dst, to, sem = gs.at[k, at_z(4)[0], j - 4], hr.at[k, j - 4, 2], 2 * side, h_r.at[k, j - 4]
        else:
            src, dst, to, sem = hs.at[k, j - 6], gr.at[k, j - 4], 2 * side, g_r.at[k]
        return remote(src, dst, g_s, sem, at_z(to)[1])

    def far_copy(j):
        half = pl.ds(j * (tok // 2), tok // 2)
        return remote(far.at[half, :], via.at[j], f_s, f_r.at[j], at_x(1 if j == 0 else 3)[1])

    def near_copy(q, j):
        here = pl.ds(q * quarter, quarter)
        return remote(bs.at[j, here, :], br.at[j, here, :], b_s, b_r.at[q], at_x(1 if j == 0 else 3)[1])

    def c_copy(k, j):
        return remote(cs.at[k], cr.at[k, x], c_s, c_r.at[k], at_x(XOFF[j])[1])

    def q_copy(j):
        return remote(sqs, sqr.at[x], q_s, q_r, at_x(XOFF[j])[1])

    def y_copy(j):
        return remote(us, ty.at[x * GROUP + me], y_s, y_r, at_all(*ALL[j]))

    def z_copy(j):
        return remote(ts, tz.at[z], z_s, z_r, at_z(ZOFF[j])[1])

    def positions():
        row = ids[...]
        col = jnp.broadcast_to(row, (128, tok)).T[:, 0:1]
        before = lax.broadcasted_iota(i32, (tok, 1), 0) < lax.broadcasted_iota(i32, (1, tok), 1)
        rank = jnp.sum(jnp.where((col == row) & before, 1, 0), axis=0, keepdims=True)
        k, core = row & (NK - 1), (row >> 2) & (NC - 1)
        zz, yy = (row >> 3) & (NZ - 1), row >> 6
        pos = ((k * GROUP + yy * NC + core) * MOST + rank) * NZ + zz
        posr[...] = pos
        posc[...] = jnp.broadcast_to(pos, (128, tok)).T

    def gather(k):
        rows = lax.broadcasted_iota(i32, (nrow, 1), 0) + k * nrow
        hot = jnp.where(rows == posr[...], 1.0, 0.0).astype(bf16)
        snd[k] = nn(hot, xg[...]).astype(bf16).reshape(GROUP, CHUNK, 2 * fw)
        rcv[k, me] = snd[k, me]

    def send_tokens(k):
        for j in range(len(EX)):
            ex_copy(k, j).start()

    def frozen_of(dx, here):
        xx = at_x(dx)[0]
        return nt(xg[here, fw : 2 * fw], w[pl.ds(pl.multiple_of(xx * fw, fw), fw), :])

    def frozen_far():
        far[...] = frozen_of(2, slice(None)).astype(bf16)
        for j in range(2):
            far_copy(j).start()

    def frozen_near(q):
        here = pl.ds(q * quarter, quarter)
        for j in range(2):
            t = frozen_of(1 if j == 0 else 3, here)
            if q // 2 == j:
                if q % 2 == 0:
                    arrived(via.at[j], f_r.at[j])
                t = t + via[j, pl.ds((q % 2) * quarter, quarter), :].astype(f32)
            bs[j, here, :] = t.astype(bf16)
            near_copy(q, j).start()

    def ag_ways(k, s):
        return [up for up in (True, False) if s < 3 or up == (k % 2 == 0)]

    def ag_pass(k, s):
        for up in ag_ways(k, s):
            if s > 0:
                ag_copy(k, s - 1, up).wait_recv()
            ag_copy(k, s, up).start()

    def ag_end(k):
        for up in (True, False):
            ag_copy(k, 3 if up in ag_ways(k, 3) else 2, up).wait_recv()

    lane = lax.broadcasted_iota(i32, (1, NZ, NZ * R), 2) // R
    sub = lax.broadcasted_iota(i32, (1, NZ, NZ * R), 1)
    mine = lane == sub

    def rows_of(k, first):
        return rcv[k, :, :, first : first + fw].reshape(nrow, fw)

    def project(k):
        pulled = nt(rows_of(k, fw), adb[k, :, 1].reshape(NZ * R, fw)).reshape(GROUP * MOST, NZ, NZ * R)
        projected = nt(rows_of(k, 0), adb[k, :, 0].reshape(NZ * R, fw)).reshape(GROUP * MOST, NZ, NZ * R)
        cs[k, 0] = jnp.sum(jnp.where(mine, pulled, 0.0), axis=1)
        cs[k, 1] = jnp.sum(jnp.where(mine, projected, 0.0), axis=1)
        cr[k, x] = cs[k]
        for j in range(len(XOFF)):
            c_copy(k, j).start()

    def gradients(k):
        low = (cr[k, 0] + cr[k, 1] + cr[k, 2] + cr[k, 3]).astype(bf16).astype(f32)
        pull = jnp.where(mine, low[0][:, None, :], 0.0).reshape(nrow, NZ * R)
        proj = jnp.where(mine, low[1][:, None, :], 0.0).reshape(nrow, NZ * R)
        for i, (side, first) in enumerate(((pull, 0), (proj, fw))):
            grad = (adapter_scale * nn(side.T.astype(bf16), rows_of(k, first))).reshape(NZ, R, fw)
            gf[:, i] = grad
            gs[k, :, i] = grad.astype(bf16)
        for j in (2, 3, 4, 5, 0, 1):
            g_copy(k, j).start()
        gown[k] = gf[z]
        lora = adapter_scale * nn(pull.astype(bf16), adb[k, :, 0].reshape(NZ * R, fw))
        ls[k] = lora.astype(bf16).reshape(GROUP, CHUNK, fw)
        for j in range(len(EX)):
            lora_copy(k, j).start()
        lr[k, me] = ls[k, me]

    def hub(k):
        for side in range(2):
            arrived(hr.at[k, side], h_r.at[k, side])
            sign = 1 if side == 0 else -1
            for i in range(2):
                t = gf[at_z(2 * sign)[0], i] + hr[k, side, i].astype(f32)
                if i == side:
                    t = t + hr[k, side, 2].astype(f32)
                hs[k, side, i] = t.astype(bf16)
            g_copy(k, 6 + side).start()

    def unslot(k):
        cols = lax.broadcasted_iota(i32, (1, nrow), 1) + k * nrow
        hot = jnp.where(posc[:, 0:1] == cols, 1.0, 0.0).astype(bf16)
        acc[...] += nn(hot, lr[k].reshape(nrow, fw))

    def total_gradient(k):
        arrived(gr.at[k], g_r.at[k])
        t = gown[k]
        for j in range(4):
            t = t + gr[k, j].astype(f32)
        gown[k] = t
        return jnp.sum(t * t)

    loads[0].wait()
    for k in range(2):
        adb[k, z] = adf[k].astype(bf16)
    for cp in loads[1:4]:
        cp.wait()
    positions()
    gather(0)
    pl.semaphore_wait(barrier, len(ZOFF) + len(ALL))
    ag_pass(0, 0)
    send_tokens(0)
    ag_pass(1, 0)
    for k in range(2, NK):
        adb[k, z] = adf[k].astype(bf16)
    for cp in loads[4:]:
        cp.wait()
    frozen_far()
    ag_pass(0, 1)
    ag_pass(2, 0)
    gather(1)
    send_tokens(1)
    ag_pass(1, 1)
    ag_pass(3, 0)
    gather(2)
    send_tokens(2)
    ag_pass(0, 2)
    ag_pass(2, 1)
    gather(3)
    send_tokens(3)
    ag_pass(1, 2)
    ag_pass(3, 1)
    acc[...] = frozen_of(0, slice(None))
    ag_pass(0, 3)
    frozen_near(0)
    ag_pass(2, 2)
    ag_pass(1, 3)
    ag_end(0)

    for k in range(NK):
        if k > 0:
            ag_end(k)
        arrived(rcv.at[k, 0 : GROUP - 1], ex_r.at[k])
        project(k)
        if k + 1 < NK:
            frozen_near(k + 1)
        if k == 0:
            ag_pass(3, 2)
            ag_pass(2, 3)
            ag_pass(3, 3)
        else:
            hub(k - 1)
        arrived(cr.at[k, 0 : NX - 1], c_r.at[k])
        gradients(k)

    def frozen(q):
        here = pl.ds(q * quarter, quarter)
        arrived(br.at[:, here, :], b_r.at[q])
        t = acc[here, :]
        for j in range(2):
            t = t + br[j, here, :].astype(f32)
        acc[here, :] = t

    def lora_wait(k):
        arrived(lr.at[k, 0 : GROUP - 1], l_r.at[k])

    frozen(0)
    frozen(1)
    lora_wait(0)
    unslot(0)
    hub(NK - 1)
    frozen(2)
    lora_wait(1)
    unslot(1)
    row = lax.broadcasted_iota(i32, (8, 128), 0)
    sq = jnp.zeros((8, 128), f32)
    for k in range(NK):
        sq = sq + jnp.where(row == k, total_gradient(k), 0.0)
    sqs[...] = sq
    ts[...] = jnp.sum(sq, axis=0, keepdims=True)
    for j in range(len(ZOFF)):
        z_copy(j).start()
    for j in range(len(XOFF)):
        q_copy(j).start()
    sqr[x] = sq
    tz[z] = ts[...]
    frozen(3)
    arrived(tz.at[0 : NZ - 1], z_r)
    us[...] = jnp.sum(tz[...], axis=0)
    for j in range(len(ALL)):
        y_copy(j).start()
    ty[x * GROUP + me] = us[...]
    lora_wait(2)
    unslot(2)
    arrived(sqr.at[0 : NX - 1], q_r)
    squares = sqr[0] + sqr[1] + sqr[2] + sqr[3]
    for k in range(NK):
        factor = clip_limit / jnp.maximum(jnp.sqrt(squares[k : k + 1, 0:1]), clip_limit)
        clipped = gown[k] * factor
        new_first = beta_first * mb[k] + (1.0 - beta_first) * clipped
        new_second = beta_second * vb[k] + (1.0 - beta_second) * clipped * clipped
        update = new_first / bias_first / (jnp.sqrt(new_second / bias_second) + adam_eps)
        adf[k] = adf[k] - learn_rate * update
        mb[k] = new_first
        vb[k] = new_second
    moved = [
        pltpu.make_async_copy(src, dst, osem.at[i + 1])
        for i, (src, dst) in enumerate(((adf, na_hbm), (mb, nf_hbm), (vb, ns_hbm)))
    ]
    for cp in moved:
        cp.start()
    lora_wait(3)
    unslot(3)
    obf[...] = acc[...].astype(bf16)
    out_copy = pltpu.make_async_copy(obf, out_hbm, osem.at[0])
    out_copy.start()
    left(snd.at[:, 0 : GROUP - 1], ex_s)
    left(ls.at[:, 0 : GROUP - 1], l_s)
    left(adb.at[:, 0 : NZ - 1], ag_s)
    left(gs.at[:, 0 : NZ - 1], g_s)
    left(bs, b_s)
    left(far, f_s)
    left(cr.at[:, 0 : NX - 1], c_s)
    left(sqr.at[0 : NX - 1], q_s)
    left(tz.at[0 : NZ - 1], z_s)
    arrived(ty.at[0 : len(ALL)], y_r)
    st_ref[...] = jnp.sum(ty[...], axis=0)
    left(ty.at[0 : len(ALL)], y_s)
    for cp in (out_copy, *moved):
        cp.wait()


def finish(o_in, na_in, nf_in, ns_in, st_ref, o_out, na_out, nf_out, ns_out, norm_ref, sem):
    moves = [
        pltpu.make_async_copy(src, dst, sem.at[i])
        for i, (src, dst) in enumerate(((na_in, na_out), (nf_in, nf_out), (ns_in, ns_out), (o_in, o_out)))
    ]
    for cp in moves:
        cp.start()
    norm_ref[...] = jnp.sqrt(st_ref[0:1, 0:1])
    for cp in moves:
        cp.wait()


def local(inputs, cotangent, base_weight, adapter_ids, adapters, first_moment, second_moment):
    tok, fw = inputs.shape
    dma = pltpu.SemaphoreType.DMA
    vm, hbm, anywhere = (pl.BlockSpec(memory_space=m) for m in (pltpu.VMEM, pltpu.HBM, pl.ANY))
    own = (NK, 2, R, fw)
    results = (
        jax.ShapeDtypeStruct((tok, fw), bf16),
        jax.ShapeDtypeStruct(own, f32),
        jax.ShapeDtypeStruct(own, f32),
        jax.ShapeDtypeStruct(own, f32),
    )
    *parts, stats = pl.pallas_call(
        kernel,
        out_shape=(*results, jax.ShapeDtypeStruct((1, 128), f32)),
        in_specs=[hbm] * 7,
        out_specs=(anywhere,) * 4 + (vm,),
        scratch_shapes=[
            pltpu.VMEM(own, f32),
            pltpu.VMEM(own, f32),
            pltpu.VMEM(own, f32),
            pltpu.VMEM((1, tok), i32),
            pltpu.VMEM((1, tok), i32),
            pltpu.VMEM((tok, 128), i32),
            pltpu.VMEM((tok, 2 * fw), bf16),
            pltpu.VMEM(base_weight.shape, bf16),
            pltpu.VMEM((NK, GROUP, CHUNK, 2 * fw), bf16),
            pltpu.VMEM((NK, GROUP, CHUNK, 2 * fw), bf16),
            pltpu.VMEM((NK, NZ, 2, R, fw), bf16),
            pltpu.VMEM((tok, fw), bf16),
            pltpu.VMEM((2, tok // 2, fw), bf16),
            pltpu.VMEM((2, tok, fw), bf16),
            pltpu.VMEM((2, tok, fw), bf16),
            pltpu.VMEM((tok, fw), f32),
            pltpu.VMEM((NK, 2, GROUP * MOST, NZ * R), f32),
            pltpu.VMEM((NK, NX, 2, GROUP * MOST, NZ * R), f32),
            pltpu.VMEM((NK, GROUP, CHUNK, fw), bf16),
            pltpu.VMEM((NK, GROUP, CHUNK, fw), bf16),
            pltpu.VMEM((NK, NZ, 2, R, fw), bf16),
            pltpu.VMEM((NZ, 2, R, fw), f32),
            pltpu.VMEM((NK, 2, 2, R, fw), bf16),
            pltpu.VMEM((NK, 2, 3, R, fw), bf16),
            pltpu.VMEM((NK, 4, 2, R, fw), bf16),
            pltpu.VMEM(own, f32),
            pltpu.VMEM((tok, fw), bf16),
            pltpu.VMEM((8, 128), f32),
            pltpu.VMEM((NX, 8, 128), f32),
            pltpu.VMEM((1, 128), f32),
            pltpu.VMEM((NX * GROUP, 1, 128), f32),
            pltpu.VMEM((1, 128), f32),
            pltpu.VMEM((NZ, 1, 128), f32),
            dma((7,)), dma((4,)),
            dma, dma((NK,)),
            dma, dma((NK, 8)),
            dma, dma((2,)),
            dma, dma((NK,)),
            dma, dma((NK,)),
            dma, dma((NK,)),
            dma, dma((NK,)), dma((NK, 2)),
            dma, dma,
            dma, dma,
            dma, dma,
        ],
        compiler_params=pltpu.CompilerParams(
            collective_id=0, has_side_effects=True, vmem_limit_bytes=46 * 1024 * 1024
        ),
    )(*(pltpu.with_memory_space_constraint(t, pltpu.HBM) for t in (adapter_ids.reshape(1, tok), inputs, cotangent, base_weight, adapters, first_moment, second_moment)))
    out, new_adapters, new_first, new_second, norm = pl.pallas_call(
        finish,
        out_shape=(*results, jax.ShapeDtypeStruct((1, 1), f32)),
        in_specs=[anywhere] * 4 + [vm],
        out_specs=(hbm,) * 4 + (vm,),
        scratch_shapes=[dma((4,))],
        compiler_params=pltpu.CompilerParams(vmem_limit_bytes=8 * 1024 * 1024),
    )(*parts, stats)
    return (out, new_adapters, new_first, new_second, norm.reshape(()))


def solution(mesh):
    in_specs = (
        P("aa", "ba"),
        P("aa", "ba"),
        P(None, "ba"),
        P("aa", None),
        P("aa", None, None, "ba"),
        P("aa", None, None, "ba"),
        P("aa", None, None, "ba"),
    )
    out_specs = (
        P("aa", "ba"),
        P("aa", None, None, "ba"),
        P("aa", None, None, "ba"),
        P("aa", None, None, "ba"),
        P(),
    )
    return jax.shard_map(local, mesh=mesh, in_specs=in_specs, out_specs=out_specs, check_vma=False)
```

```python
import math

import jax
import jax.numpy as jnp
from jax import lax
from jax.experimental import pallas as pl
from jax.experimental.pallas import tpu as pltpu
from jax.sharding import PartitionSpec as P

MODEL_WIDTH = 3584
R = 16
NY, NZ, NC, NX = 4, 8, 2, 4
NK = 4
MOST = 4
GROUP = NY * NC
CHUNK = NZ * MOST
MESH = pl.DeviceIdType.MESH

adapter_scale = 2.0
beta_first = 0.9
beta_second = 0.999
adam_eps = 1e-08
learn_rate = 0.01
clip_limit = math.sqrt(2.0 * R * MODEL_WIDTH)
bias_first = 1.0 - math.exp(1000.0 * math.log(beta_first))
bias_second = 1.0 - math.exp(1000.0 * math.log(beta_second))

EX = ((2, 0), (1, 0), (3, 0), (2, 1), (1, 1), (3, 1), (0, None))
ZOFF = (4, 3, 5, 2, 6, 1, 7)
XOFF = (2, 1, 3)
ALL = tuple((dy, dc, dx) for dy in (2, 1, 3, 0) for dx in (2, 1, 3, 0) for dc in (1, 0) if (dy, dc, dx) != (0, 0, 0))
f32, bf16, i32 = jnp.float32, jnp.bfloat16, jnp.int32


def nt(a, b):
    return lax.dot_general(a, b, (((1,), (1,)), ((), ())), preferred_element_type=f32)


def nn(a, b):
    return jnp.dot(a, b, preferred_element_type=f32)


def kernel(
    ids_hbm, x_hbm, g_hbm, w_hbm, ad_hbm, m_hbm, v_hbm,
    out_hbm, na_hbm, nf_hbm, ns_hbm, st_ref,
    adf, mb, vb, ids, posr, posc, xg, w, snd, rcv, adb, far, via, bs, br, acc, cs, cr, ls, lr, gs, gf, hs, hr, gr, gown, obf,
    sqs, sqr, ts, ty, us, tz,
    lsem, osem, ex_s, ex_r, ag_s, ag_r, f_s, f_r, b_s, b_r, c_s, c_r, l_s, l_r, g_s, g_r, h_r, q_s, q_r, y_s, y_r, z_s, z_r,
):
    a = lax.axis_index("aa")
    x = lax.axis_index("ba")
    y, z, c = a // (NZ * NC), (a // NC) % NZ, a % NC
    me = y * NC + c
    tok, fw = x_hbm.shape
    nrow = GROUP * CHUNK
    quarter = tok // NK

    def at_yc(dy, core):
        yy, cc = (y + dy) % NY, 1 - c if core is None else core
        return yy * NC + cc, ((yy * NZ + z) * NC + cc, x)

    def at_z(dz):
        zz = (z + dz + NZ) % NZ
        return zz, ((y * NZ + zz) * NC + c, x)

    def at_all(dy, dc, dx):
        yy, cc = (y + dy) % NY, (c + dc) % NC
        return (yy * NZ + z) * NC + cc, (x + dx) % NX

    def at_x(dx):
        xx = (x + dx) % NX
        return xx, (a, xx)

    barrier = pltpu.get_barrier_semaphore()
    for dz in ZOFF:
        pl.semaphore_signal(barrier, inc=1, device_id=at_z(dz)[1], device_id_type=MESH)
    for step in ALL:
        pl.semaphore_signal(barrier, inc=1, device_id=at_all(*step), device_id_type=MESH)

    loads = [
        pltpu.make_async_copy(ad_hbm, adf, lsem.at[0]),
        pltpu.make_async_copy(ids_hbm, ids, lsem.at[4]),
        pltpu.make_async_copy(x_hbm, xg.at[:, 0:fw], lsem.at[1]),
        pltpu.make_async_copy(g_hbm, xg.at[:, fw : 2 * fw], lsem.at[2]),
        pltpu.make_async_copy(w_hbm, w, lsem.at[3]),
        pltpu.make_async_copy(m_hbm, mb, lsem.at[5]),
        pltpu.make_async_copy(v_hbm, vb, lsem.at[6]),
    ]
    for cp in loads:
        cp.start()

    def remote(src, dst, ssem, rsem, dev):
        return pltpu.make_async_remote_copy(
            src_ref=src, dst_ref=dst, send_sem=ssem, recv_sem=rsem, device_id=dev, device_id_type=MESH
        )

    def arrived(ref, sem):
        remote(ref, ref, sem, sem, at_x(1)[1]).wait_recv()

    def left(ref, sem):
        remote(ref, ref, sem, sem, at_x(1)[1]).wait_send()

    def ex_copy(k, j):
        d, dev = at_yc(*EX[j])
        return remote(snd.at[k, d], rcv.at[k, me], ex_s, ex_r.at[k], dev)

    def lora_copy(k, j):
        d, dev = at_yc(*EX[j])
        return remote(ls.at[k, d], lr.at[k, me], l_s, l_r.at[k], dev)

    def ag_copy(k, s, up):
        o, i = at_z(-s if up else s)[0], s if up else 4 + s
        return remote(adb.at[k, o], adb.at[k, o], ag_s, ag_r.at[k, i], at_z(1 if up else -1)[1])

    def g_copy(k, j):
        side = 1 if j % 2 == 0 else -1
        if j < 2:
            src, dst, to, sem = gs.at[k, at_z(side)[0]], gr.at[k, j], side, g_r.at[k]
        elif j < 4:
            src, dst, to, sem = gs.at[k, at_z(3 * side)[0]], hr.at[k, j - 2, 0:2], side, h_r.at[k, j - 2]
        elif j < 6:
            src, dst, to, sem = gs.at[k, at_z(4)[0], j - 4], hr.at[k, j - 4, 2], 2 * side, h_r.at[k, j - 4]
        else:
            src, dst, to, sem = hs.at[k, j - 6], gr.at[k, j - 4], 2 * side, g_r.at[k]
        return remote(src, dst, g_s, sem, at_z(to)[1])

    def far_copy(j):
        half = pl.ds(j * (tok // 2), tok // 2)
        return remote(far.at[half, :], via.at[j], f_s, f_r.at[j], at_x(1 if j == 0 else 3)[1])

    def near_copy(q, j):
        here = pl.ds(q * quarter, quarter)
        return remote(bs.at[j, here, :], br.at[j, here, :], b_s, b_r.at[q], at_x(1 if j == 0 else 3)[1])

    def c_copy(k, j):
        return remote(cs.at[k], cr.at[k, x], c_s, c_r.at[k], at_x(XOFF[j])[1])

    def q_copy(j):
        return remote(sqs, sqr.at[x], q_s, q_r, at_x(XOFF[j])[1])

    def y_copy(j):
        return remote(us, ty.at[x * GROUP + me], y_s, y_r, at_all(*ALL[j]))

    def z_copy(j):
        return remote(ts, tz.at[z], z_s, z_r, at_z(ZOFF[j])[1])

    def positions():
        row = ids[...]
        col = jnp.broadcast_to(row, (128, tok)).T[:, 0:1]
        before = lax.broadcasted_iota(i32, (tok, 1), 0) < lax.broadcasted_iota(i32, (1, tok), 1)
        rank = jnp.sum(jnp.where((col == row) & before, 1, 0), axis=0, keepdims=True)
        k, core = row & (NK - 1), (row >> 2) & (NC - 1)
        zz, yy = (row >> 3) & (NZ - 1), row >> 6
        pos = ((k * GROUP + yy * NC + core) * MOST + rank) * NZ + zz
        posr[...] = pos
        posc[...] = jnp.broadcast_to(pos, (128, tok)).T

    def gather(k):
        rows = lax.broadcasted_iota(i32, (nrow, 1), 0) + k * nrow
        hot = jnp.where(rows == posr[...], 1.0, 0.0).astype(bf16)
        snd[k] = nn(hot, xg[...]).astype(bf16).reshape(GROUP, CHUNK, 2 * fw)
        rcv[k, me] = snd[k, me]

    def send_tokens(k):
        for j in range(len(EX)):
            ex_copy(k, j).start()

    def frozen_of(dx, here):
        xx = at_x(dx)[0]
        return nt(xg[here, fw : 2 * fw], w[pl.ds(pl.multiple_of(xx * fw, fw), fw), :])

    def frozen_far():
        far[...] = frozen_of(2, slice(None)).astype(bf16)
        for j in range(2):
            far_copy(j).start()

    def frozen_near(q):
        here = pl.ds(q * quarter, quarter)
        for j in range(2):
            t = frozen_of(1 if j == 0 else 3, here)
            if q // 2 == j:
                if q % 2 == 0:
                    arrived(via.at[j], f_r.at[j])
                t = t + via[j, pl.ds((q % 2) * quarter, quarter), :].astype(f32)
            bs[j, here, :] = t.astype(bf16)
            near_copy(q, j).start()

    def ag_ways(k, s):
        return [up for up in (True, False) if s < 3 or up == (k % 2 == 0)]

    def ag_pass(k, s):
        for up in ag_ways(k, s):
            if s > 0:
                ag_copy(k, s - 1, up).wait_recv()
            ag_copy(k, s, up).start()

    def ag_end(k):
        for up in (True, False):
            ag_copy(k, 3 if up in ag_ways(k, 3) else 2, up).wait_recv()

    lane = lax.broadcasted_iota(i32, (1, NZ, NZ * R), 2) // R
    sub = lax.broadcasted_iota(i32, (1, NZ, NZ * R), 1)
    mine = lane == sub

    def rows_of(k, first):
        return rcv[k, :, :, first : first + fw].reshape(nrow, fw)

    def project(k):
        pulled = nt(rows_of(k, fw), adb[k, :, 1].reshape(NZ * R, fw)).reshape(GROUP * MOST, NZ, NZ * R)
        projected = nt(rows_of(k, 0), adb[k, :, 0].reshape(NZ * R, fw)).reshape(GROUP * MOST, NZ, NZ * R)
        cs[k, 0] = jnp.sum(jnp.where(mine, pulled, 0.0), axis=1)
        cs[k, 1] = jnp.sum(jnp.where(mine, projected, 0.0), axis=1)
        cr[k, x] = cs[k]
        for j in range(len(XOFF)):
            c_copy(k, j).start()

    def gradients(k):
        low = (cr[k, 0] + cr[k, 1] + cr[k, 2] + cr[k, 3]).astype(bf16).astype(f32)
        pull = jnp.where(mine, low[0][:, None, :], 0.0).reshape(nrow, NZ * R)
        proj = jnp.where(mine, low[1][:, None, :], 0.0).reshape(nrow, NZ * R)
        for i, (side, first) in enumerate(((pull, 0), (proj, fw))):
            grad = (adapter_scale * nn(side.T.astype(bf16), rows_of(k, first))).reshape(NZ, R, fw)
            gf[k % 2, :, i] = grad
            gs[k, :, i] = grad.astype(bf16)
        for j in (2, 3, 4, 5, 0, 1):
            g_copy(k, j).start()
        gown[k] = gf[k % 2, z]
        lora = adapter_scale * nn(pull.astype(bf16), adb[k, :, 0].reshape(NZ * R, fw))
        ls[k] = lora.astype(bf16).reshape(GROUP, CHUNK, fw)
        for j in range(len(EX)):
            lora_copy(k, j).start()
        lr[k, me] = ls[k, me]

    def hub(k):
        for side in range(2):
            arrived(hr.at[k, side], h_r.at[k, side])
            sign = 1 if side == 0 else -1
            for i in range(2):
                t = gf[k % 2, at_z(2 * sign)[0], i] + hr[k, side, i].astype(f32)
                if i == side:
                    t = t + hr[k, side, 2].astype(f32)
                hs[k, side, i] = t.astype(bf16)
            g_copy(k, 6 + side).start()

    def unslot(k):
        cols = lax.broadcasted_iota(i32, (1, nrow), 1) + k * nrow
        hot = jnp.where(posc[:, 0:1] == cols, 1.0, 0.0).astype(bf16)
        acc[...] += nn(hot, lr[k].reshape(nrow, fw))

    def total_gradient(k):
        arrived(gr.at[k], g_r.at[k])
        t = gown[k]
        for j in range(4):
            t = t + gr[k, j].astype(f32)
        gown[k] = t
        return jnp.sum(t * t)

    loads[0].wait()
    for k in range(2):
        adb[k, z] = adf[k].astype(bf16)
    for cp in loads[1:4]:
        cp.wait()
    positions()
    gather(0)
    pl.semaphore_wait(barrier, len(ZOFF) + len(ALL))
    ag_pass(0, 0)
    send_tokens(0)
    ag_pass(1, 0)
    for k in range(2, NK):
        adb[k, z] = adf[k].astype(bf16)
    for cp in loads[4:]:
        cp.wait()
    frozen_far()
    ag_pass(0, 1)
    ag_pass(2, 0)
    gather(1)
    send_tokens(1)
    ag_pass(1, 1)
    ag_pass(3, 0)
    gather(2)
    send_tokens(2)
    ag_pass(0, 2)
    ag_pass(2, 1)
    gather(3)
    send_tokens(3)
    ag_pass(1, 2)
    ag_pass(3, 1)
    acc[...] = frozen_of(0, slice(None))
    ag_pass(0, 3)
    frozen_near(0)
    ag_pass(2, 2)
    ag_pass(1, 3)
    ag_end(0)

    for k in range(NK):
        if k > 0:
            ag_end(k)
        arrived(rcv.at[k, 0 : GROUP - 1], ex_r.at[k])
        project(k)
        if k + 1 < NK:
            frozen_near(k + 1)
        if k == 0:
            ag_pass(3, 2)
            ag_pass(2, 3)
            ag_pass(3, 3)
        elif k < NK - 1:
            hub(k - 1)
        arrived(cr.at[k, 0 : NX - 1], c_r.at[k])
        gradients(k)
        if k == NK - 1:
            hub(k - 1)

    def frozen(q):
        here = pl.ds(q * quarter, quarter)
        arrived(br.at[:, here, :], b_r.at[q])
        t = acc[here, :]
        for j in range(2):
            t = t + br[j, here, :].astype(f32)
        acc[here, :] = t

    def lora_wait(k):
        arrived(lr.at[k, 0 : GROUP - 1], l_r.at[k])

    frozen(0)
    frozen(1)
    lora_wait(0)
    unslot(0)
    hub(NK - 1)
    frozen(2)
    lora_wait(1)
    unslot(1)
    row = lax.broadcasted_iota(i32, (8, 128), 0)
    sq = jnp.zeros((8, 128), f32)
    for k in range(NK):
        sq = sq + jnp.where(row == k, total_gradient(k), 0.0)
    sqs[...] = sq
    ts[...] = jnp.sum(sq, axis=0, keepdims=True)
    for j in range(len(ZOFF)):
        z_copy(j).start()
    for j in range(len(XOFF)):
        q_copy(j).start()
    sqr[x] = sq
    tz[z] = ts[...]
    frozen(3)
    arrived(tz.at[0 : NZ - 1], z_r)
    us[...] = jnp.sum(tz[...], axis=0)
    for j in range(len(ALL)):
        y_copy(j).start()
    ty[x * GROUP + me] = us[...]
    lora_wait(2)
    unslot(2)
    arrived(sqr.at[0 : NX - 1], q_r)
    squares = sqr[0] + sqr[1] + sqr[2] + sqr[3]
    for k in range(NK):
        factor = clip_limit / jnp.maximum(jnp.sqrt(squares[k : k + 1, 0:1]), clip_limit)
        clipped = gown[k] * factor
        new_first = beta_first * mb[k] + (1.0 - beta_first) * clipped
        new_second = beta_second * vb[k] + (1.0 - beta_second) * clipped * clipped
        update = new_first / bias_first / (jnp.sqrt(new_second / bias_second) + adam_eps)
        adf[k] = adf[k] - learn_rate * update
        mb[k] = new_first
        vb[k] = new_second
    moved = [
        pltpu.make_async_copy(src, dst, osem.at[i + 1])
        for i, (src, dst) in enumerate(((adf, na_hbm), (mb, nf_hbm), (vb, ns_hbm)))
    ]
    for cp in moved:
        cp.start()
    lora_wait(3)
    unslot(3)
    obf[...] = acc[...].astype(bf16)
    out_copy = pltpu.make_async_copy(obf, out_hbm, osem.at[0])
    out_copy.start()
    left(snd.at[:, 0 : GROUP - 1], ex_s)
    left(ls.at[:, 0 : GROUP - 1], l_s)
    left(adb.at[:, 0 : NZ - 1], ag_s)
    left(gs.at[:, 0 : NZ - 1], g_s)
    left(bs, b_s)
    left(far, f_s)
    left(cr.at[:, 0 : NX - 1], c_s)
    left(sqr.at[0 : NX - 1], q_s)
    left(tz.at[0 : NZ - 1], z_s)
    arrived(ty.at[0 : len(ALL)], y_r)
    st_ref[...] = jnp.sum(ty[...], axis=0)
    left(ty.at[0 : len(ALL)], y_s)
    for cp in (out_copy, *moved):
        cp.wait()


def finish(o_in, na_in, nf_in, ns_in, st_ref, o_out, na_out, nf_out, ns_out, norm_ref, sem):
    moves = [
        pltpu.make_async_copy(src, dst, sem.at[i])
        for i, (src, dst) in enumerate(((na_in, na_out), (nf_in, nf_out), (ns_in, ns_out), (o_in, o_out)))
    ]
    for cp in moves:
        cp.start()
    norm_ref[...] = jnp.sqrt(st_ref[0:1, 0:1])
    for cp in moves:
        cp.wait()


def local(inputs, cotangent, base_weight, adapter_ids, adapters, first_moment, second_moment):
    tok, fw = inputs.shape
    dma = pltpu.SemaphoreType.DMA
    vm, hbm, anywhere = (pl.BlockSpec(memory_space=m) for m in (pltpu.VMEM, pltpu.HBM, pl.ANY))
    own = (NK, 2, R, fw)
    results = (
        jax.ShapeDtypeStruct((tok, fw), bf16),
        jax.ShapeDtypeStruct(own, f32),
        jax.ShapeDtypeStruct(own, f32),
        jax.ShapeDtypeStruct(own, f32),
    )
    *parts, stats = pl.pallas_call(
        kernel,
        out_shape=(*results, jax.ShapeDtypeStruct((1, 128), f32)),
        in_specs=[hbm] * 7,
        out_specs=(anywhere,) * 4 + (vm,),
        scratch_shapes=[
            pltpu.VMEM(own, f32),
            pltpu.VMEM(own, f32),
            pltpu.VMEM(own, f32),
            pltpu.VMEM((1, tok), i32),
            pltpu.VMEM((1, tok), i32),
            pltpu.VMEM((tok, 128), i32),
            pltpu.VMEM((tok, 2 * fw), bf16),
            pltpu.VMEM(base_weight.shape, bf16),
            pltpu.VMEM((NK, GROUP, CHUNK, 2 * fw), bf16),
            pltpu.VMEM((NK, GROUP, CHUNK, 2 * fw), bf16),
            pltpu.VMEM((NK, NZ, 2, R, fw), bf16),
            pltpu.VMEM((tok, fw), bf16),
            pltpu.VMEM((2, tok // 2, fw), bf16),
            pltpu.VMEM((2, tok, fw), bf16),
            pltpu.VMEM((2, tok, fw), bf16),
            pltpu.VMEM((tok, fw), f32),
            pltpu.VMEM((NK, 2, GROUP * MOST, NZ * R), f32),
            pltpu.VMEM((NK, NX, 2, GROUP * MOST, NZ * R), f32),
            pltpu.VMEM((NK, GROUP, CHUNK, fw), bf16),
            pltpu.VMEM((NK, GROUP, CHUNK, fw), bf16),
            pltpu.VMEM((NK, NZ, 2, R, fw), bf16),
            pltpu.VMEM((2, NZ, 2, R, fw), f32),
            pltpu.VMEM((NK, 2, 2, R, fw), bf16),
            pltpu.VMEM((NK, 2, 3, R, fw), bf16),
            pltpu.VMEM((NK, 4, 2, R, fw), bf16),
            pltpu.VMEM(own, f32),
            pltpu.VMEM((tok, fw), bf16),
            pltpu.VMEM((8, 128), f32),
            pltpu.VMEM((NX, 8, 128), f32),
            pltpu.VMEM((1, 128), f32),
            pltpu.VMEM((NX * GROUP, 1, 128), f32),
            pltpu.VMEM((1, 128), f32),
            pltpu.VMEM((NZ, 1, 128), f32),
            dma((7,)), dma((4,)),
            dma, dma((NK,)),
            dma, dma((NK, 8)),
            dma, dma((2,)),
            dma, dma((NK,)),
            dma, dma((NK,)),
            dma, dma((NK,)),
            dma, dma((NK,)), dma((NK, 2)),
            dma, dma,
            dma, dma,
            dma, dma,
        ],
        compiler_params=pltpu.CompilerParams(
            collective_id=0, has_side_effects=True, vmem_limit_bytes=46 * 1024 * 1024
        ),
    )(*(pltpu.with_memory_space_constraint(t, pltpu.HBM) for t in (adapter_ids.reshape(1, tok), inputs, cotangent, base_weight, adapters, first_moment, second_moment)))
    out, new_adapters, new_first, new_second, norm = pl.pallas_call(
        finish,
        out_shape=(*results, jax.ShapeDtypeStruct((1, 1), f32)),
        in_specs=[anywhere] * 4 + [vm],
        out_specs=(hbm,) * 4 + (vm,),
        scratch_shapes=[dma((4,))],
        compiler_params=pltpu.CompilerParams(vmem_limit_bytes=8 * 1024 * 1024),
    )(*parts, stats)
    return (out, new_adapters, new_first, new_second, norm.reshape(()))


def solution(mesh):
    in_specs = (
        P("aa", "ba"),
        P("aa", "ba"),
        P(None, "ba"),
        P("aa", None),
        P("aa", None, None, "ba"),
        P("aa", None, None, "ba"),
        P("aa", None, None, "ba"),
    )
    out_specs = (
        P("aa", "ba"),
        P("aa", None, None, "ba"),
        P("aa", None, None, "ba"),
        P("aa", None, None, "ba"),
        P(),
    )
    return jax.shard_map(local, mesh=mesh, in_specs=in_specs, out_specs=out_specs, check_vma=False)
```
